128 devices in a mesh: trade: 16 (over z, x), path: 8 (over y, core).
Axes of the slice: x: 4, y: 4, z: 4, core: 2. Of those that a mesh axis runs over, the one named last changes fastest.
Arguments:
- coefficients: bfloat16 [32768, 256], P('trade'), may hold values from -6 to 6
- path_basis: bfloat16 [256, 4096], P(None, 'path'), may hold values from -6 to 6
- trade_owner: int32 [32768, 1], P('trade'), may hold values from 0 to 15; in each aligned block of 2048 rows (0 to 2047, 2048 to 4095, ...) at most 192 rows name the same one
- trade_slot: int32 [32768], P('trade'), may hold values from 0 to 63
- set_factor: int32 [1024], P('trade'), may hold values from 0 to 511
- set_level: int32 [1024], P('trade'), may hold values from 0 to 3
- default_date: int32 [512, 4096], P(None, 'path'), may hold values from 0 to 4
- discount: float32 [4], replicated, may hold values from 0.5 to 1
Outputs:
- alloc: float32 [32768], P('trade')
- set_cva: float32 [1024], P('trade')
The draws below stay inside these ranges and needn't reach their ends.
Inputs may be any that keep to these rules, and one draw needn't show every extreme that they name: `trade_owner`: in the rows of one device no value is named by more than 192 rows, a bound that some block reaches.
All inputs are finite; a program needn't handle non-finite values.
Results may differ from the reference program's by a relative error of at most 0.0045.
Values may be sent and summed in bfloat16 or wider, within the bound.
A program may use at most 64 MiB of HBM per device.

```python
import math
import jax
import jax.numpy as jnp
import numpy as np

K = 64
CREDIT = 512
DATES = 4
TR_DEV = 2048
NS_DEV = 64
TRADES = 32768
PATHS = 4096
NSETS = 1024
CAP = 192
N_TRADE = 16


def place_ends(result, stream_key, low, high):
    place = [jax.random.randint(jax.random.fold_in(stream_key, axis), (), 0, length) for axis, length in enumerate(result.shape)]
    longest = result.shape.index(max(result.shape))
    neighbour = place[:longest] + [(place[longest] + 1) % result.shape[longest]] + place[longest + 1:]
    return result.at[tuple(place)].set(low).at[tuple(neighbour)].set(high)


def levels(stream_key, dims, cuts, low, high):
    factor_of = 1.0
    for axis_at, blocks in cuts:
        heights = jax.random.uniform(jax.random.fold_in(jax.random.fold_in(stream_key, 6), axis_at), (blocks,), jnp.float32, low / len(cuts), high / len(cuts))
        factor_of = factor_of * jnp.repeat(jnp.exp(heights), dims[axis_at] // blocks).reshape((-1,) + (1,) * (len(dims) - 1 - axis_at))
    return factor_of


def deal_out(key, own, number, rows, count, top, reach, skew):
    order = jax.random.permutation(key, count)
    crowded, ordinary = portions_of(count, rows * top, reach, skew, True), portions_of(count, rows * top, reach, skew, False)
    places = jnp.arange(count)

    def named(lengths, offset_by):
        used = int((lengths > 0).sum())
        fixed = max(1, used // 4)
        passed = fixed + (places - fixed + offset_by * (used - fixed)) % max(1, count - fixed)
        return jnp.zeros((count,), jnp.int32).at[order[jnp.where(places < fixed, places, passed)]].set(jnp.asarray(lengths, jnp.int32))

    lengths = jnp.where(number % 4 == 0, named(crowded, number // 4), named(ordinary, number - number // 4 - 1))
    mixed = jax.random.permutation(jax.random.fold_in(own, 3), count)
    giver, receiver = mixed[0:count // 2 * 2:2], mixed[1:count // 2 * 2:2]
    margin = jnp.minimum(lengths[giver] - 1, reach - lengths[receiver]) // 2
    margin = jnp.where((giver == order[0]) | (receiver == order[0]) | (lengths[receiver] == 0), 0, jnp.maximum(margin, 0))
    passed = jax.random.randint(jax.random.fold_in(own, 4), (count // 2,), 0, 1 << 20) % (margin + 1)
    lengths = lengths.at[giver].add(-passed).at[receiver].add(passed)
    labels = jnp.searchsorted(jnp.cumsum(lengths), jnp.arange(rows * top), side="right").astype(jnp.int32)
    listing = labels.reshape(top, rows).T
    listing = listing[jax.random.permutation(jax.random.fold_in(own, 1), rows)]
    offset_by = jax.random.randint(jax.random.fold_in(own, 2), (rows, 1), 0, top)
    return jnp.take_along_axis(listing, (jnp.arange(top)[None, :] + offset_by) % top, axis=1)


def portions_of(number_of, total, bound, slope, full):
    weights = [(1 << 20) // math.isqrt(grade ** slope) + 1 for grade in range(1, number_of + 1)]
    largest = bound if full else min(bound, max(-(-total // number_of), total * weights[0] // sum(weights)))
    least = 1 if total - largest >= number_of - 1 else 0
    given, rest = [largest] + [least] * (number_of - 1), total - largest - least * (number_of - 1)
    while rest > 0:
        free = [i for i in range(1, number_of) if given[i] < largest] or [i for i in range(1, number_of) if given[i] < bound]
        whole, left = sum([weights[i] for i in free]), rest
        for i in free:
            more = min(bound - given[i], max(1, left * weights[i] // whole), rest)
            given[i] = given[i] + more
            rest = rest - more
    return np.array(given)


def centred(rng, extent, scale, limit, split=(), dtype=jnp.bfloat16):
    entries = scale * jax.random.normal(rng, extent, jnp.float32)
    if split:
        entries = entries * levels(rng, extent, split, -0.22, 0.18)
    return jnp.clip(entries, -limit, limit).astype(dtype)


def setup_inputs(seed: int = 0) -> dict:
    splits = jax.random.split(jax.random.key(seed), 9)
    coefficients = centred(splits[0], (TRADES, DATES * K), 1.0, 6.0, ((0, 16),))
    path_basis = centred(splits[1], (DATES * K, PATHS), 1.0, 6.0, ((1, 8),))
    trade_owner_keys = jax.random.split(jax.random.fold_in(splits[2], 1), TRADES // TR_DEV)
    trade_owner_turns = jax.random.permutation(jax.random.fold_in(splits[2], 3), TRADES // TR_DEV)
    trade_owner = jax.vmap(lambda own, number: deal_out(jax.random.fold_in(splits[2], 2), own, number, TR_DEV, N_TRADE, 1, CAP, 2))(trade_owner_keys, trade_owner_turns).reshape((TRADES, 1))
    trade_slot = place_ends(jax.random.randint(splits[3], (TRADES,), 0, NS_DEV), jax.random.fold_in(splits[3], 1), 0, NS_DEV - 1).astype(jnp.int32)
    set_factor = place_ends(jax.random.randint(splits[4], (NSETS,), 0, CREDIT), jax.random.fold_in(splits[4], 1), 0, CREDIT - 1).astype(jnp.int32)
    set_level = place_ends(jax.random.randint(splits[5], (NSETS,), 0, 4), jax.random.fold_in(splits[5], 1), 0, 3).astype(jnp.int32)
    default_date = place_ends(jax.random.randint(splits[6], (CREDIT, PATHS), 0, DATES + 1), jax.random.fold_in(splits[6], 1), 0, DATES).astype(jnp.int32)
    discount = jnp.clip(jnp.exp(jax.random.uniform(splits[7], (DATES,), jnp.float32, math.log(0.5), math.log(1.0))), 0.5, 1.0)
    return {"coefficients": coefficients, "path_basis": path_basis, "trade_owner": trade_owner, "trade_slot": trade_slot, "set_factor": set_factor, "set_level": set_level, "default_date": default_date, "discount": discount}


level_step = 1.5


def reference(coefficients, path_basis, trade_owner, trade_slot, set_factor, set_level, default_date, discount):
    set_of = (trade_owner[:, 0] * NS_DEV + trade_slot).astype(jnp.int32)
    threshold = level_step * set_level.astype(jnp.float32)
    set_cva = jnp.zeros((NSETS,), jnp.float32)
    alloc = jnp.zeros((TRADES,), jnp.float32)
    for moment in range(DATES):
        values = jnp.dot(coefficients[:, moment * K:(moment + 1) * K], path_basis[moment * K:(moment + 1) * K, :], preferred_element_type=jnp.float32).astype(jnp.bfloat16)
        netted = jax.ops.segment_sum(values.astype(jnp.float32), set_of, num_segments=NSETS)
        excess = netted - threshold[:, None]
        struck = (default_date == moment).astype(jnp.float32)
        defaulted = struck[set_factor]
        weight = defaulted * (discount[moment] / PATHS)
        set_cva = set_cva + jnp.sum(weight * jax.nn.softplus(excess), axis=1)
        slopes = (weight * jax.nn.sigmoid(excess)).astype(jnp.bfloat16)
        alloc = alloc + jnp.sum(slopes[set_of].astype(jnp.float32) * values.astype(jnp.float32), axis=1)
    return alloc, set_cva
```

```python
import jax
import jax.numpy as jnp
from jax import lax
from jax.experimental import pallas as pl
from jax.experimental.pallas import tpu as pltpu
from jax.sharding import PartitionSpec as P

MESH = pl.DeviceIdType.MESH
K = 64
DATES = 4
LANES = 128
level_step = 1.5


def grid_offsets(side):
    def far(step):
        return min(step, side - step)

    offsets = [(a, b) for a in range(side) for b in range(side) if a or b]
    return sorted(offsets, key=lambda o: -(far(o[0]) + far(o[1])))


def column_of(row, size):
    eye = lax.broadcasted_iota(jnp.int32, (size, size), 0) == lax.broadcasted_iota(
        jnp.int32, (size, size), 1
    )
    return jnp.sum(jnp.where(eye, row, 0.0), axis=1, keepdims=True)


def row_of(column, size):
    eye = lax.broadcasted_iota(jnp.int32, (size, size), 0) == lax.broadcasted_iota(
        jnp.int32, (size, size), 1
    )
    return jnp.sum(jnp.where(eye, column, 0.0), axis=0, keepdims=True)


def make_kernel(n_trade, n_path, side, n_set, trades, per_path, factors):
    half = n_set // 2
    rows = n_trade * half
    width = DATES * K
    offsets = grid_offsets(side)
    path_steps = sorted(range(1, n_path), key=lambda k: -min(k, n_path - k))

    def kernel(
        coef_hbm, basis_hbm, owner_hbm, slot_hbm, factor_hbm, level_hbm, date_hbm, disc_hbm,
        alloc_ref, cva_ref,
        coef, basis, owner, slot, factor, level, date, disc,
        onehot, part, arrived, net, gpart, gother, gall, cva_mine, cva_in, al_mine, al_in,
        in_sem, s1, r1, sd, rd, s3, r3, sc, rc, sa, ra,
    ):
        me = lax.axis_index("trade")
        lane = lax.axis_index("path")
        core = lax.rem(lane, 2)
        partner = lane + 1 - 2 * core
        me_a, me_b = me // side, lax.rem(me, side)
        others = [
            lax.rem(me_a + a, side) * side + lax.rem(me_b + b, side) for a, b in offsets
        ]
        on_path = [lax.rem(lane + k, n_path) for k in path_steps]

        loads = [
            pltpu.make_async_copy(src, dst, in_sem.at[i])
            for i, (src, dst) in enumerate(
                (
                    (owner_hbm, owner), (slot_hbm, slot), (coef_hbm, coef), (basis_hbm, basis),
                    (factor_hbm, factor), (level_hbm, level), (disc_hbm, disc), (date_hbm, date),
                )
            )
        ]
        for load in loads:
            load.start()

        barrier = pltpu.get_barrier_semaphore()
        for o in others:
            pl.semaphore_signal(barrier, inc=1, device_id={"trade": o}, device_id_type=MESH)
        for q in on_path:
            pl.semaphore_signal(barrier, inc=1, device_id={"path": q}, device_id_type=MESH)

        loads[0].wait()
        loads[1].wait()
        loc = slot[...] - half * core
        ids = jnp.where((loc >= 0) & (loc < half), owner[...] * half + loc, -1)
        which = lax.broadcasted_iota(jnp.int32, (rows, LANES), 0)
        for r in range(trades // LANES):
            hit = which == ids[r : r + 1, :]
            onehot[:, r * LANES : (r + 1) * LANES] = jnp.where(hit, 1.0, 0.0).astype(jnp.bfloat16)
        loads[2].wait()
        sums = jnp.dot(onehot[...], coef[...], preferred_element_type=jnp.float32)
        part[...] = sums.astype(jnp.bfloat16).reshape(n_trade, half, width)

        pl.semaphore_wait(barrier, len(others) + len(on_path))
        sends = []
        firsts = []
        for j, o in enumerate(others):
            copy = pltpu.make_async_remote_copy(
                src_ref=part.at[o], dst_ref=arrived.at[j], send_sem=s1.at[j], recv_sem=r1.at[j],
                device_id={"trade": o}, device_id_type=MESH,
            )
            copy.start()
            firsts.append(copy)

        loads[4].wait()
        loads[5].wait()
        loads[6].wait()
        limit = level_step * column_of(level[...].astype(jnp.float32), n_set)
        wanted = column_of(factor[...].astype(jnp.float32), n_set)
        pick = (
            lax.broadcasted_iota(jnp.int32, (n_set, factors), 1).astype(jnp.float32) == wanted
        )
        pick = jnp.where(pick, 1.0, 0.0).astype(jnp.bfloat16)
        loads[7].wait()
        dated = jnp.dot(
            pick, date[...].astype(jnp.float32).astype(jnp.bfloat16),
            preferred_element_type=jnp.float32,
        )
        loads[3].wait()

        total = part[me].astype(jnp.float32)
        for j, copy in enumerate(firsts):
            copy.wait_recv()
            total = total + arrived[j].astype(jnp.float32)
        net[core] = total
        swap = pltpu.make_async_remote_copy(
            src_ref=net.at[core], dst_ref=net.at[core], send_sem=sd.at[0], recv_sem=rd.at[0],
            device_id={"path": partner}, device_id_type=MESH,
        )
        swap.start()
        swap.wait_recv()
        sends.append(swap)

        both = net[...].reshape(n_set, width)
        high = both.astype(jnp.bfloat16)
        low = (both - high.astype(jnp.float32)).astype(jnp.bfloat16)
        moment_of = lax.broadcasted_iota(jnp.int32, (n_set, width), 1) // K
        zero = jnp.zeros_like(high)
        b = basis[...]
        stack_high = jnp.concatenate([jnp.where(moment_of == d, high, zero) for d in range(DATES)])
        stack_low = jnp.concatenate([jnp.where(moment_of == d, low, zero) for d in range(DATES)])
        netted = jnp.dot(stack_high, b, preferred_element_type=jnp.float32) + jnp.dot(
            stack_low, b, preferred_element_type=jnp.float32
        )
        cva = jnp.zeros((n_set, 1), jnp.float32)
        slopes = []
        for d in range(DATES):
            x = netted[d * n_set : (d + 1) * n_set] - limit
            e = jnp.exp(-jnp.abs(x))
            inv = 1.0 / (1.0 + e)
            plus = jnp.maximum(x, 0.0) + jnp.log1p(e)
            sig = jnp.where(x >= 0, inv, e * inv)
            factor_d = disc[0:1, d : d + 1] / (per_path * n_path)
            weight = jnp.where(dated == float(d), factor_d, 0.0)
            cva = cva + jnp.sum(weight * plus, axis=1, keepdims=True)
            slopes.append((weight * sig).astype(jnp.bfloat16))
        grads = lax.dot_general(
            jnp.concatenate(slopes), b, (((1,), (1,)), ((), ())),
            preferred_element_type=jnp.float32,
        )
        grad = jnp.zeros((n_set, width), jnp.float32)
        for d in range(DATES):
            grad = grad + jnp.where(moment_of == d, grads[d * n_set : (d + 1) * n_set], 0.0)
        gpart[...] = grad.reshape(2, half, width)
        swap = pltpu.make_async_remote_copy(
            src_ref=gpart.at[1 - core], dst_ref=gother, send_sem=sd.at[1], recv_sem=rd.at[1],
            device_id={"path": partner}, device_id_type=MESH,
        )
        swap.start()
        sends.append(swap)
        cva_mine[...] = row_of(cva, n_set)
        cvas = []
        for j, q in enumerate(on_path):
            copy = pltpu.make_async_remote_copy(
                src_ref=cva_mine, dst_ref=cva_in.at[j], send_sem=sc.at[j], recv_sem=rc.at[j],
                device_id={"path": q}, device_id_type=MESH,
            )
            cvas.append(copy)
        swap.wait_recv()
        gall[me] = (gpart[core] + gother[...]).astype(jnp.bfloat16)
        seconds = []
        for j, o in enumerate(others):
            copy = pltpu.make_async_remote_copy(
                src_ref=gall.at[me], dst_ref=gall.at[me], send_sem=s3.at[j], recv_sem=r3.at[j],
                device_id={"trade": o}, device_id_type=MESH,
            )
            copy.start()
            seconds.append(copy)
        for copy in cvas:
            copy.start()
        for copy in seconds:
            copy.wait_recv()

        g = gall[...].reshape(rows, width)
        block = 2 * LANES
        for r in range(trades // block):
            dots = lax.dot_general(
                g, coef[r * block : (r + 1) * block, :], (((1,), (1,)), ((), ())),
                preferred_element_type=jnp.float32,
            )
            for h in range(2):
                at = 2 * r + h
                hit = which == ids[at : at + 1, :]
                al_mine[at : at + 1, :] = jnp.sum(
                    jnp.where(hit, dots[:, h * LANES : (h + 1) * LANES], 0.0),
                    axis=0, keepdims=True,
                )
        lasts = []
        for j, q in enumerate(on_path):
            copy = pltpu.make_async_remote_copy(
                src_ref=al_mine, dst_ref=al_in.at[j], send_sem=sa.at[j], recv_sem=ra.at[j],
                device_id={"path": q}, device_id_type=MESH,
            )
            copy.start()
            lasts.append(copy)
        cva_total = cva_mine[...]
        for j, copy in enumerate(cvas):
            copy.wait_recv()
            cva_total = cva_total + cva_in[j]
        cva_ref[...] = cva_total
        for copy in firsts + sends + seconds + cvas:
            copy.wait_send()
        total_alloc = al_mine[...]
        for j, copy in enumerate(lasts):
            copy.wait_recv()
            total_alloc = total_alloc + al_in[j]
        alloc_ref[...] = total_alloc
        for copy in lasts:
            copy.wait_send()

    return kernel


def solution(mesh):
    n_trade, n_path = mesh.shape["trade"], mesh.shape["path"]
    side = 4

    def on_device(
        coefficients, path_basis, trade_owner, trade_slot, set_factor, set_level, default_date,
        discount,
    ):
        trades, width = coefficients.shape
        n_set = set_factor.shape[0]
        factors, per_path = default_date.shape
        half = n_set // 2
        tall = trades // LANES
        bf16, f32, i32 = jnp.bfloat16, jnp.float32, jnp.int32
        dma = pltpu.SemaphoreType.DMA
        alloc, cva = pl.pallas_call(
            make_kernel(n_trade, n_path, side, n_set, trades, per_path, factors),
            out_shape=(
                jax.ShapeDtypeStruct((tall, LANES), f32),
                jax.ShapeDtypeStruct((1, n_set), f32),
            ),
            in_specs=[pl.BlockSpec(memory_space=pl.ANY)] * 8,
            out_specs=(
                pl.BlockSpec(memory_space=pltpu.VMEM),
                pl.BlockSpec(memory_space=pltpu.VMEM),
            ),
            scratch_shapes=[
                pltpu.VMEM((trades, width), bf16),
                pltpu.VMEM((width, per_path), bf16),
                pltpu.VMEM((tall, LANES), i32),
                pltpu.VMEM((tall, LANES), i32),
                pltpu.VMEM((1, n_set), i32),
                pltpu.VMEM((1, n_set), i32),
                pltpu.VMEM((factors, per_path), i32),
                pltpu.VMEM((1, DATES), f32),
                pltpu.VMEM((n_trade * half, trades), bf16),
                pltpu.VMEM((n_trade, half, width), bf16),
                pltpu.VMEM((n_trade - 1, half, width), bf16),
                pltpu.VMEM((2, half, width), f32),
                pltpu.VMEM((2, half, width), f32),
                pltpu.VMEM((half, width), f32),
                pltpu.VMEM((n_trade, half, width), bf16),
                pltpu.VMEM((1, n_set), f32),
                pltpu.VMEM((n_path - 1, 1, n_set), f32),
                pltpu.VMEM((tall, LANES), f32),
                pltpu.VMEM((n_path - 1, tall, LANES), f32),
                dma((8,)),
                dma((n_trade - 1,)),
                dma((n_trade - 1,)),
                dma((2,)),
                dma((2,)),
                dma((n_trade - 1,)),
                dma((n_trade - 1,)),
                dma((n_path - 1,)),
                dma((n_path - 1,)),
                dma((n_path - 1,)),
                dma((n_path - 1,)),
            ],
            compiler_params=pltpu.CompilerParams(collective_id=0, has_side_effects=True),
        )(
            coefficients,
            path_basis,
            trade_owner.reshape(tall, LANES),
            trade_slot.reshape(tall, LANES),
            set_factor.reshape(1, n_set),
            set_level.reshape(1, n_set),
            default_date,
            discount.reshape(1, DATES),
        )
        return alloc.reshape(trades), cva.reshape(n_set)

    return jax.shard_map(
        on_device,
        mesh=mesh,
        in_specs=(
            P("trade", None),
            P(None, "path"),
            P("trade", None),
            P("trade"),
            P("trade"),
            P("trade"),
            P(None, "path"),
            P(),
        ),
        out_specs=(P("trade"), P("trade")),
        check_vma=False,
    )
```

```python
import jax
import jax.numpy as jnp
from jax import lax
from jax.experimental import pallas as pl
from jax.experimental.pallas import tpu as pltpu
from jax.sharding import PartitionSpec as P

MESH = pl.DeviceIdType.MESH
K = 64
DATES = 4
LANES = 128
level_step = 1.5


def grid_offsets(side):
    def far(step):
        return min(step, side - step)

    offsets = [(a, b) for a in range(side) for b in range(side) if a or b]
    return sorted(offsets, key=lambda o: -(far(o[0]) + far(o[1])))


def diagonal(rows, columns, first):
    at = lax.broadcasted_iota(jnp.int32, (rows, columns), 0) + first
    return at == lax.broadcasted_iota(jnp.int32, (rows, columns), 1)


def make_kernel(n_trade, n_path, side, n_set, trades, per_path, factors):
    half = n_set // 2
    rows = n_trade * half
    width = DATES * K
    offsets = grid_offsets(side)
    path_steps = sorted(range(1, n_path), key=lambda k: -min(k, n_path - k))

    def kernel(
        coef_hbm, basis_hbm, owner_hbm, slot_hbm, factor_hbm, level_hbm, date_hbm, disc_hbm,
        alloc_ref, cva_ref,
        coef, basis, basis_other, owner, slot, factor, level, date, disc,
        onehot, part, arrived, dated, dated_other, gall, cva_mine, cva_in, al_mine, al_in,
        in_sem, s1, r1, sd, rd, s3, r3, sc, rc, sa, ra,
    ):
        me = lax.axis_index("trade")
        lane = lax.axis_index("path")
        core = lax.rem(lane, 2)
        partner = lane + 1 - 2 * core
        me_a, me_b = me // side, lax.rem(me, side)
        others = [
            lax.rem(me_a + a, side) * side + lax.rem(me_b + b, side) for a, b in offsets
        ]
        on_path = [lax.rem(lane + k, n_path) for k in path_steps]

        barrier = pltpu.get_barrier_semaphore()
        for o in others:
            pl.semaphore_signal(barrier, inc=1, device_id={"trade": o}, device_id_type=MESH)
        for q in on_path:
            pl.semaphore_signal(barrier, inc=1, device_id={"path": q}, device_id_type=MESH)
        loads = [
            pltpu.make_async_copy(src, dst, in_sem.at[i])
            for i, (src, dst) in enumerate(
                (
                    (owner_hbm, owner), (slot_hbm, slot), (coef_hbm, coef), (basis_hbm, basis),
                    (factor_hbm, factor), (level_hbm, level), (disc_hbm, disc), (date_hbm, date),
                )
            )
        ]
        for load in loads:
            load.start()

        loads[0].wait()
        loads[1].wait()
        loc = slot[...] - half * core
        ids = jnp.where((loc >= 0) & (loc < half), owner[...] * half + loc, -1)
        which = lax.broadcasted_iota(jnp.int32, (rows, LANES), 0)
        for r in range(trades // LANES):
            hit = which == ids[r : r + 1, :]
            onehot[:, r * LANES : (r + 1) * LANES] = jnp.where(hit, 1.0, 0.0).astype(jnp.bfloat16)
        loads[2].wait()
        sums = jnp.dot(onehot[...], coef[...], preferred_element_type=jnp.float32)
        part[...] = sums.astype(jnp.bfloat16).reshape(n_trade, half, width)

        loads[3].wait()
        pl.semaphore_wait(barrier, len(others) + len(on_path))
        firsts = []
        for j, o in enumerate(others):
            copy = pltpu.make_async_remote_copy(
                src_ref=part.at[o], dst_ref=arrived.at[j], send_sem=s1.at[j], recv_sem=r1.at[j],
                device_id={"trade": o}, device_id_type=MESH,
            )
            copy.start()
            firsts.append(copy)
        swap_basis = pltpu.make_async_remote_copy(
            src_ref=basis, dst_ref=basis_other, send_sem=sd.at[0], recv_sem=rd.at[0],
            device_id={"path": partner}, device_id_type=MESH,
        )
        swap_basis.start()

        loads[4].wait()
        loads[5].wait()
        loads[6].wait()
        limit = level_step * jnp.sum(
            jnp.where(diagonal(half, n_set, half * core), level[...].astype(jnp.float32), 0.0),
            axis=1, keepdims=True,
        )
        wanted = jnp.sum(
            jnp.where(diagonal(n_set, n_set, 0), factor[...].astype(jnp.float32), 0.0),
            axis=1, keepdims=True,
        )
        pick = (
            lax.broadcasted_iota(jnp.int32, (n_set, factors), 1).astype(jnp.float32) == wanted
        )
        pick = jnp.where(pick, 1.0, 0.0).astype(jnp.bfloat16)
        loads[7].wait()
        dated[...] = jnp.dot(
            pick, date[...].astype(jnp.float32).astype(jnp.bfloat16),
            preferred_element_type=jnp.float32,
        ).reshape(2, half, per_path)
        swap_dates = pltpu.make_async_remote_copy(
            src_ref=dated.at[1 - core], dst_ref=dated_other, send_sem=sd.at[1], recv_sem=rd.at[1],
            device_id={"path": partner}, device_id_type=MESH,
        )
        swap_dates.start()
        swap_basis.wait_recv()
        swap_dates.wait_recv()

        total = part[me].astype(jnp.float32)
        for j in reversed(range(len(firsts))):
            firsts[j].wait_recv()
            total = total + arrived[j].astype(jnp.float32)

        high = total.astype(jnp.bfloat16)
        low = (total - high.astype(jnp.float32)).astype(jnp.bfloat16)
        moment_of = lax.broadcasted_iota(jnp.int32, (half, width), 1) // K
        zero = jnp.zeros_like(high)
        stack_high = jnp.concatenate([jnp.where(moment_of == d, high, zero) for d in range(DATES)])
        stack_low = jnp.concatenate([jnp.where(moment_of == d, low, zero) for d in range(DATES)])
        cva = jnp.zeros((half, 1), jnp.float32)
        grads = 0.0
        for b_ref, when in ((basis, dated[core]), (basis_other, dated_other[...])):
            b = b_ref[...]
            netted = jnp.dot(stack_high, b, preferred_element_type=jnp.float32) + jnp.dot(
                stack_low, b, preferred_element_type=jnp.float32
            )
            slopes = []
            for d in range(DATES):
                x = netted[d * half : (d + 1) * half] - limit
                e = jnp.exp(-jnp.abs(x))
                inv = 1.0 / (1.0 + e)
                plus = jnp.maximum(x, 0.0) + jnp.log1p(e)
                sig = jnp.where(x >= 0, inv, e * inv)
                factor_d = disc[0:1, d : d + 1] / (per_path * n_path)
                weight = jnp.where(when == float(d), factor_d, 0.0)
                cva = cva + jnp.sum(weight * plus, axis=1, keepdims=True)
                slopes.append((weight * sig).astype(jnp.bfloat16))
            grads = grads + lax.dot_general(
                jnp.concatenate(slopes), b, (((1,), (1,)), ((), ())),
                preferred_element_type=jnp.float32,
            )
        grad = jnp.zeros((half, width), jnp.float32)
        for d in range(DATES):
            grad = grad + jnp.where(moment_of == d, grads[d * half : (d + 1) * half], 0.0)
        gall[me] = grad.astype(jnp.bfloat16)
        seconds = []
        for j, o in enumerate(others):
            copy = pltpu.make_async_remote_copy(
                src_ref=gall.at[me], dst_ref=gall.at[me], send_sem=s3.at[j], recv_sem=r3.at[j],
                device_id={"trade": o}, device_id_type=MESH,
            )
            copy.start()
            seconds.append(copy)
        cva_mine[...] = jnp.sum(
            jnp.where(diagonal(half, n_set, half * core), cva, 0.0), axis=0, keepdims=True
        )
        cvas = []
        for j, q in enumerate(on_path):
            copy = pltpu.make_async_remote_copy(
                src_ref=cva_mine, dst_ref=cva_in.at[j], send_sem=sc.at[j], recv_sem=rc.at[j],
                device_id={"path": q}, device_id_type=MESH,
            )
            copy.start()
            cvas.append(copy)
        for copy in reversed(seconds):
            copy.wait_recv()

        g = gall[...].reshape(rows, width)
        block = 2 * LANES
        for r in range(trades // block):
            dots = lax.dot_general(
                g, coef[r * block : (r + 1) * block, :], (((1,), (1,)), ((), ())),
                preferred_element_type=jnp.float32,
            )
            for h in range(2):
                at = 2 * r + h
                hit = which == ids[at : at + 1, :]
                al_mine[at : at + 1, :] = jnp.sum(
                    jnp.where(hit, dots[:, h * LANES : (h + 1) * LANES], 0.0),
                    axis=0, keepdims=True,
                )
        lasts = []
        for j, q in enumerate(on_path):
            copy = pltpu.make_async_remote_copy(
                src_ref=al_mine, dst_ref=al_in.at[j], send_sem=sa.at[j], recv_sem=ra.at[j],
                device_id={"path": q}, device_id_type=MESH,
            )
            copy.start()
            lasts.append(copy)
        cva_total = cva_mine[...]
        for j, copy in enumerate(cvas):
            copy.wait_recv()
            cva_total = cva_total + cva_in[j]
        cva_ref[...] = cva_total
        for copy in firsts + [swap_basis, swap_dates] + seconds + cvas:
            copy.wait_send()
        total_alloc = al_mine[...]
        for j in reversed(range(len(lasts))):
            lasts[j].wait_recv()
            total_alloc = total_alloc + al_in[j]
        alloc_ref[...] = total_alloc
        for copy in lasts:
            copy.wait_send()

    return kernel


def write_out(alloc, cva, alloc_out, cva_out, sem):
    copies = [
        pltpu.make_async_copy(src, dst, sem.at[i])
        for i, (src, dst) in enumerate(((alloc, alloc_out), (cva, cva_out)))
    ]
    for copy in copies:
        copy.start()
    for copy in copies:
        copy.wait()


def solution(mesh):
    n_trade, n_path = mesh.shape["trade"], mesh.shape["path"]
    side = 4

    def on_device(
        coefficients, path_basis, trade_owner, trade_slot, set_factor, set_level, default_date,
        discount,
    ):
        trades, width = coefficients.shape
        n_set = set_factor.shape[0]
        factors, per_path = default_date.shape
        half = n_set // 2
        tall = trades // LANES
        bf16, f32, i32 = jnp.bfloat16, jnp.float32, jnp.int32
        dma = pltpu.SemaphoreType.DMA
        alloc, cva = pl.pallas_call(
            make_kernel(n_trade, n_path, side, n_set, trades, per_path, factors),
            out_shape=(pltpu.VMEM((tall, LANES), f32), pltpu.VMEM((1, n_set), f32)),
            in_specs=[pl.BlockSpec(memory_space=pl.ANY)] * 8,
            out_specs=(
                pl.BlockSpec(memory_space=pltpu.VMEM),
                pl.BlockSpec(memory_space=pltpu.VMEM),
            ),
            scratch_shapes=[
                pltpu.VMEM((trades, width), bf16),
                pltpu.VMEM((width, per_path), bf16),
                pltpu.VMEM((width, per_path), bf16),
                pltpu.VMEM((tall, LANES), i32),
                pltpu.VMEM((tall, LANES), i32),
                pltpu.VMEM((1, n_set), i32),
                pltpu.VMEM((1, n_set), i32),
                pltpu.VMEM((factors, per_path), i32),
                pltpu.VMEM((1, DATES), f32),
                pltpu.VMEM((n_trade * half, trades), bf16),
                pltpu.VMEM((n_trade, half, width), bf16),
                pltpu.VMEM((n_trade - 1, half, width), bf16),
                pltpu.VMEM((2, half, per_path), f32),
                pltpu.VMEM((half, per_path), f32),
                pltpu.VMEM((n_trade, half, width), bf16),
                pltpu.VMEM((1, n_set), f32),
                pltpu.VMEM((n_path - 1, 1, n_set), f32),
                pltpu.VMEM((tall, LANES), f32),
                pltpu.VMEM((n_path - 1, tall, LANES), f32),
                dma((8,)),
                dma((n_trade - 1,)),
                dma((n_trade - 1,)),
                dma((2,)),
                dma((2,)),
                dma((n_trade - 1,)),
                dma((n_trade - 1,)),
                dma((n_path - 1,)),
                dma((n_path - 1,)),
                dma((n_path - 1,)),
                dma((n_path - 1,)),
            ],
            compiler_params=pltpu.CompilerParams(collective_id=0, has_side_effects=True),
        )(
            coefficients,
            path_basis,
            trade_owner.reshape(tall, LANES),
            trade_slot.reshape(tall, LANES),
            set_factor.reshape(1, n_set),
            set_level.reshape(1, n_set),
            default_date,
            discount.reshape(1, DATES),
        )
        alloc, cva = pl.pallas_call(
            write_out,
            out_shape=(
                jax.ShapeDtypeStruct((tall, LANES), f32),
                jax.ShapeDtypeStruct((1, n_set), f32),
            ),
            in_specs=[pl.BlockSpec(memory_space=pltpu.VMEM)] * 2,
            out_specs=(
                pl.BlockSpec(memory_space=pltpu.HBM),
                pl.BlockSpec(memory_space=pltpu.HBM),
            ),
            scratch_shapes=[dma((2,))],
            compiler_params=pltpu.CompilerParams(vmem_limit_bytes=1 << 20),
        )(alloc, cva)
        return alloc.reshape(trades), cva.reshape(n_set)

    return jax.shard_map(
        on_device,
        mesh=mesh,
        in_specs=(
            P("trade", None),
            P(None, "path"),
            P("trade", None),
            P("trade"),
            P("trade"),
            P("trade"),
            P(None, "path"),
            P(),
        ),
        out_specs=(P("trade"), P("trade")),
        check_vma=False,
    )
```

```python
import jax
import jax.numpy as jnp
from jax import lax
from jax.experimental import pallas as pl
from jax.experimental.pallas import tpu as pltpu
from jax.sharding import PartitionSpec as P

MESH = pl.DeviceIdType.MESH
K = 64
DATES = 4
LANES = 128
level_step = 1.5


def grid_offsets(side):
    def far(step):
        return min(step, side - step)

    offsets = [(a, b) for a in range(side) for b in range(side)]
    return sorted(offsets, key=lambda o: -(far(o[0]) + far(o[1])))


def diagonal(rows, columns, first):
    at = lax.broadcasted_iota(jnp.int32, (rows, columns), 0) + first
    return at == lax.broadcasted_iota(jnp.int32, (rows, columns), 1)


def arrive(ref, sem):
    pltpu.make_async_copy(ref, ref, sem).wait()


def turned(x):
    size = x.shape[1]
    ones = jnp.where(diagonal(size, size, 0), 1.0, 0.0).astype(x.dtype)
    return lax.dot_general(
        ones, x, (((1,), (1,)), ((), ())), preferred_element_type=jnp.float32
    ).astype(x.dtype)


def make_kernel(n_trade, n_path, side, n_set, trades, per_path, factors):
    offsets = grid_offsets(side)
    n_along = n_path - 1
    count = n_set // 2
    sub = count // 2
    rows = n_trade * sub
    width = DATES * K
    path_steps = sorted(range(1, n_path), key=lambda k: -min(k, n_path - k))
    early = n_trade // 2 + 1
    tall = trades // LANES
    f32, bf16 = jnp.float32, jnp.bfloat16

    def kernel(
        coef_hbm, basis_hbm, owner_hbm, slot_hbm, factor_hbm, level_hbm, date_hbm, disc_hbm,
        alloc_ref, cva_ref,
        coef, coef_t, basis, basis_other, basis_t, where, sets, date, disc, onehot, dated, dated_other,
        cva_mine, cva_in, al_mine, al_in, part, arrived, gmine, gall,
        in_sem, s1, r1, sd, rd, s3, r3, sc, rc, sa, ra,
    ):
        me = lax.axis_index("trade")
        lane = lax.axis_index("path")
        core = lax.rem(lane, 2)
        partner = lane + 1 - 2 * core
        me_a, me_b = me // side, lax.rem(me, side)
        others = [
            lax.rem(me_a + a, side) * side + lax.rem(me_b + b, side) for a, b in offsets
        ]
        on_path = [lax.rem(lane + k, n_path) for k in path_steps]

        across = [{"trade": o, "path": partner} for o in others]
        first, first_sent = count * core, count * (1 - core)

        barrier = pltpu.get_barrier_semaphore()
        for there in across:
            pl.semaphore_signal(barrier, inc=1, device_id=there, device_id_type=MESH)
        for k, q in zip(path_steps, on_path):
            if k % 2 == 0:
                pl.semaphore_signal(barrier, inc=1, device_id={"path": q}, device_id_type=MESH)
        for y in range(1, n_path // 2):
            q = lax.rem(partner + 2 * y, n_path)
            pl.semaphore_signal(barrier, inc=1, device_id={"path": q}, device_id_type=MESH)
        for src, dst, i in (
            (owner_hbm, where.at[0], 0), (slot_hbm, where.at[1], 0), (coef_hbm, coef, 1),
            (basis_hbm, basis, 2), (factor_hbm, sets.at[0], 3), (level_hbm, sets.at[1], 3),
            (disc_hbm, disc, 4), (date_hbm, date, 5),
        ):
            pltpu.make_async_copy(src, dst, in_sem.at[i]).start()

        def send(src, dst, send_sem, recv_sem, device):
            pltpu.make_async_remote_copy(
                src_ref=src, dst_ref=dst, send_sem=send_sem, recv_sem=recv_sem,
                device_id=device, device_id_type=MESH,
            ).start()

        arrive(where, in_sem.at[0])
        loc = where[1] - first_sent
        ids = jnp.where(
            (loc >= 0) & (loc < count), (loc // sub) * rows + where[0] * sub + lax.rem(loc, sub), -1
        )
        which = lax.broadcasted_iota(jnp.int32, (2 * rows, LANES), 0)
        for r in range(tall):
            hit = which == ids[r : r + 1, :]
            onehot[:, r * LANES : (r + 1) * LANES] = jnp.where(hit, 1.0, 0.0).astype(bf16)
        arrive(coef, in_sem.at[1])
        sums = jnp.dot(onehot[...], coef[...], preferred_element_type=f32)
        part[...] = sums.astype(bf16).reshape(2, n_trade, sub, width)

        arrive(basis, in_sem.at[2])
        pl.semaphore_wait(barrier, n_trade + n_path - 2)
        for h in range(2):
            for j, (o, there) in enumerate(zip(others, across)):
                group = 0 if j < early else 1
                send(part.at[h, o], arrived.at[h, j], s1.at[0], r1.at[2 * h + group], there)
        send(basis, basis_other, sd.at[0], rd.at[0], {"path": partner})

        arrive(sets, in_sem.at[3])
        arrive(disc, in_sem.at[4])
        limit = level_step * jnp.sum(
            jnp.where(diagonal(count, n_set, first), sets[1].astype(f32), 0.0),
            axis=1, keepdims=True,
        )
        wanted = jnp.sum(
            jnp.where(diagonal(n_set, n_set, 0), sets[0].astype(f32), 0.0),
            axis=1, keepdims=True,
        )
        pick = lax.broadcasted_iota(jnp.int32, (n_set, factors), 1).astype(f32) == wanted
        pick = jnp.where(pick, 1.0, 0.0).astype(bf16)
        arrive(date, in_sem.at[5])
        dated[...] = jnp.dot(
            pick, date[...].astype(f32).astype(bf16), preferred_element_type=f32
        ).reshape(2, count, per_path)
        send(dated.at[1 - core], dated_other, sd.at[1], rd.at[1], {"path": partner})
        coef_t[...] = turned(coef[...])
        basis_t[0] = turned(basis[...])
        arrive(basis_other, rd.at[0])
        basis_t[1] = turned(basis_other[...])
        arrive(dated_other, rd.at[1])

        moment_of = lax.broadcasted_iota(jnp.int32, (sub, width), 1) // K
        cvas = []
        for h in range(2):
            some_sets = slice(h * sub, (h + 1) * sub)
            total = jnp.zeros((sub, width), f32)
            for group, some in ((1, range(early, n_trade)), (0, range(early))):
                arrive(arrived.at[h, some.start : some.stop], r1.at[2 * h + group])
                for j in some:
                    total = total + arrived[h, j].astype(f32)
            stack = jnp.concatenate([jnp.where(moment_of == d, total, 0.0) for d in range(DATES)])
            high = stack.astype(bf16)
            low = (stack - high.astype(f32)).astype(bf16)
            cva = jnp.zeros((sub, 1), f32)
            grads = 0.0
            for i, (b_ref, when) in enumerate(
                ((basis, dated[core, some_sets]), (basis_other, dated_other[some_sets]))
            ):
                b = b_ref[...]
                netted = jnp.dot(high, b, preferred_element_type=f32) + jnp.dot(
                    low, b, preferred_element_type=f32
                )
                slopes = []
                for d in range(DATES):
                    x = netted[d * sub : (d + 1) * sub] - limit[some_sets]
                    e = jnp.exp(-jnp.abs(x))
                    inv = 1.0 / (1.0 + e)
                    plus = jnp.maximum(x, 0.0) + jnp.log1p(e)
                    sig = jnp.where(x >= 0, inv, e * inv)
                    factor_d = disc[0:1, d : d + 1] / (per_path * n_path)
                    weight = jnp.where(when == float(d), factor_d, 0.0)
                    cva = cva + jnp.sum(weight * plus, axis=1, keepdims=True)
                    slopes.append(weight * sig)
                grads = grads + jnp.dot(
                    jnp.concatenate(slopes).astype(bf16), basis_t[i], preferred_element_type=f32
                )
            cvas.append(cva)
            grad = jnp.zeros((sub, width), f32)
            for d in range(DATES):
                grad = grad + jnp.where(moment_of == d, grads[d * sub : (d + 1) * sub], 0.0)
            gmine[h] = grad.astype(bf16)
            for there in across:
                send(gmine.at[h], gall.at[h, me], s3.at[0], r3.at[h], there)
        cva = jnp.concatenate(cvas)
        cva_mine[...] = jnp.sum(
            jnp.where(diagonal(count, n_set, first), cva, 0.0), axis=0, keepdims=True
        )
        for j, q in enumerate(on_path):
            send(cva_mine, cva_in.at[j], sc.at[0], rc.at[0], {"path": q})

        block = 2 * LANES
        for h in range(2):
            arrive(gall.at[h], r3.at[h])
            g = gall[h].reshape(rows, width)
            which = lax.broadcasted_iota(jnp.int32, (rows, LANES), 0) + h * rows
            for r in range(trades // block):
                dots = jnp.dot(
                    g, coef_t[:, r * block : (r + 1) * block], preferred_element_type=f32
                )
                for i in range(2):
                    at = 2 * r + i
                    hit = which == ids[at : at + 1, :]
                    share = jnp.sum(
                        jnp.where(hit, dots[:, i * LANES : (i + 1) * LANES], 0.0),
                        axis=0, keepdims=True,
                    )
                    if h == 0:
                        al_mine[at // 8, at % 8 : at % 8 + 1, :] = share
                    else:
                        al_mine[at // 8, at % 8 : at % 8 + 1, :] += share
                if h == 1 and (2 * r + 2) % 8 == 0:
                    i = (2 * r + 2) // 8 - 1
                    for j, q in enumerate(on_path):
                        send(al_mine.at[i], al_in.at[i, j], sa.at[0], ra.at[i], {"path": q})
        arrive(arrived, s1.at[0])
        arrive(arrived, s3.at[0])
        arrive(basis, sd.at[0])
        arrive(dated_other, sd.at[1])
        arrive(cva_in, sc.at[0])


        arrive(cva_in, rc.at[0])
        cva_total = cva_mine[...]
        for j in range(n_along):
            cva_total = cva_total + cva_in[j]
        cva_ref[...] = cva_total
        for i in range(tall // 8):
            arrive(al_in.at[i], ra.at[i])
            total_alloc = al_mine[i]
            for j in range(n_along):
                total_alloc = total_alloc + al_in[i, j]
            alloc_ref[i * 8 : (i + 1) * 8] = total_alloc
        arrive(al_in, sa.at[0])

    return kernel


def write_out(alloc, cva, alloc_out, cva_out, sem):
    copies = [
        pltpu.make_async_copy(src, dst, sem.at[i])
        for i, (src, dst) in enumerate(((alloc, alloc_out), (cva, cva_out)))
    ]
    for copy in copies:
        copy.start()
    for copy in copies:
        copy.wait()


def solution(mesh):
    n_trade, n_path = mesh.shape["trade"], mesh.shape["path"]
    side = 4

    def on_device(
        coefficients, path_basis, trade_owner, trade_slot, set_factor, set_level, default_date,
        discount,
    ):
        trades, width = coefficients.shape
        n_set = set_factor.shape[0]
        factors, per_path = default_date.shape
        tall = trades // LANES
        half = n_set // 2
        bf16, f32, i32 = jnp.bfloat16, jnp.float32, jnp.int32
        dma = pltpu.SemaphoreType.DMA
        alloc, cva = pl.pallas_call(
            make_kernel(n_trade, n_path, side, n_set, trades, per_path, factors),
            out_shape=(pltpu.VMEM((tall, LANES), f32), pltpu.VMEM((1, n_set), f32)),
            in_specs=[pl.BlockSpec(memory_space=pl.ANY)] * 8,
            out_specs=(
                pl.BlockSpec(memory_space=pltpu.VMEM),
                pl.BlockSpec(memory_space=pltpu.VMEM),
            ),
            scratch_shapes=[
                pltpu.VMEM((trades, width), bf16),
                pltpu.VMEM((width, trades), bf16),
                pltpu.VMEM((width, per_path), bf16),
                pltpu.VMEM((width, per_path), bf16),
                pltpu.VMEM((2, per_path, width), bf16),
                pltpu.VMEM((2, tall, LANES), i32),
                pltpu.VMEM((2, 1, n_set), i32),
                pltpu.VMEM((factors, per_path), i32),
                pltpu.VMEM((1, DATES), f32),
                pltpu.VMEM((n_trade * half, trades), bf16),
                pltpu.VMEM((2, half, per_path), f32),
                pltpu.VMEM((half, per_path), f32),
                pltpu.VMEM((1, n_set), f32),
                pltpu.VMEM((n_path - 1, 1, n_set), f32),
                pltpu.VMEM((tall // 8, 8, LANES), f32),
                pltpu.VMEM((tall // 8, n_path - 1, 8, LANES), f32),
                pltpu.VMEM((2, n_trade, half // 2, width), bf16),
                pltpu.VMEM((2, n_trade, half // 2, width), bf16),
                pltpu.VMEM((2, half // 2, width), bf16),
                pltpu.VMEM((2, n_trade, half // 2, width), bf16),
                dma((6,)),
                dma((1,)),
                dma((4,)),
                dma((2,)),
                dma((2,)),
                dma((1,)),
                dma((2,)),
                dma((1,)),
                dma((1,)),
                dma((1,)),
                dma((2,)),
            ],
            compiler_params=pltpu.CompilerParams(collective_id=0, has_side_effects=True),
        )(
            coefficients,
            path_basis,
            trade_owner.reshape(tall, LANES),
            trade_slot.reshape(tall, LANES),
            set_factor.reshape(1, n_set),
            set_level.reshape(1, n_set),
            default_date,
            discount.reshape(1, DATES),
        )
        alloc, cva = pl.pallas_call(
            write_out,
            out_shape=(
                jax.ShapeDtypeStruct((tall, LANES), f32),
                jax.ShapeDtypeStruct((1, n_set), f32),
            ),
            in_specs=[pl.BlockSpec(memory_space=pltpu.VMEM)] * 2,
            out_specs=(
                pl.BlockSpec(memory_space=pltpu.HBM),
                pl.BlockSpec(memory_space=pltpu.HBM),
            ),
            scratch_shapes=[dma((2,))],
            compiler_params=pltpu.CompilerParams(vmem_limit_bytes=1 << 20),
        )(alloc, cva)
        return alloc.reshape(trades), cva.reshape(n_set)

    return jax.shard_map(
        on_device,
        mesh=mesh,
        in_specs=(
            P("trade", None),
            P(None, "path"),
            P("trade", None),
            P("trade"),
            P("trade"),
            P("trade"),
            P(None, "path"),
            P(),
        ),
        out_specs=(P("trade"), P("trade")),
        check_vma=False,
    )
```

```python
import jax
import jax.numpy as jnp
from jax import lax
from jax.experimental import pallas as pl
from jax.experimental.pallas import tpu as pltpu
from jax.sharding import PartitionSpec as P

MESH = pl.DeviceIdType.MESH
K = 64
DATES = 4
LANES = 128
level_step = 1.5


def grid_offsets(side):
    def far(step):
        return min(step, side - step)

    offsets = [(a, b) for a in range(side) for b in range(side)]
    return sorted(offsets, key=lambda o: (-(far(o[0]) + far(o[1])), (o[0] + 2 * o[1]) % 4, o[0]))


def diagonal(rows, columns, first):
    at = lax.broadcasted_iota(jnp.int32, (rows, columns), 0) + first
    return at == lax.broadcasted_iota(jnp.int32, (rows, columns), 1)


def arrive(ref, sem):
    pltpu.make_async_copy(ref, ref, sem).wait()


def turned(x):
    size = x.shape[1]
    ones = jnp.where(diagonal(size, size, 0), 1.0, 0.0).astype(x.dtype)
    return lax.dot_general(
        ones, x, (((1,), (1,)), ((), ())), preferred_element_type=jnp.float32
    ).astype(x.dtype)


def make_kernel(n_trade, n_path, side, n_set, trades, per_path, factors):
    offsets = grid_offsets(side)
    n_along = n_path - 1
    count = n_set // 2
    sub = count // 2
    rows = n_trade * sub
    width = DATES * K
    path_steps = sorted(range(1, n_path), key=lambda k: (2, 4, 3, 5, 6, 7, 1).index(k))
    early = n_trade // 2 + 1
    tall = trades // LANES
    f32, bf16 = jnp.float32, jnp.bfloat16

    def kernel(
        coef_hbm, basis_hbm, owner_hbm, slot_hbm, factor_hbm, level_hbm, date_hbm, disc_hbm,
        alloc_ref, cva_ref,
        coef, coef_t, basis, basis_other, basis_t, where, sets, date, disc, onehot, dated, dated_other, excess, weights,
        cva_mine, cva_in, al_mine, al_in, part, arrived, gmine, gall,
        in_sem, s1, r1, sd, rd, s3, r3, sc, rc, sa, ra,
    ):
        me = lax.axis_index("trade")
        lane = lax.axis_index("path")
        core = lax.rem(lane, 2)
        partner = lane + 1 - 2 * core
        me_a, me_b = me // side, lax.rem(me, side)
        others = [
            lax.rem(me_a + a, side) * side + lax.rem(me_b + b, side) for a, b in offsets
        ]
        on_path = [lax.rem(lane + k, n_path) for k in path_steps]

        across = [{"trade": o, "path": partner} for o in others]
        first, first_sent = count * core, count * (1 - core)

        loads = [
            pltpu.make_async_copy(src, dst, in_sem.at[i])
            for src, dst, i in (
                (owner_hbm, where.at[0], 0), (slot_hbm, where.at[1], 0), (coef_hbm, coef, 1),
                (basis_hbm, basis, 2), (factor_hbm, sets.at[0], 3), (level_hbm, sets.at[1], 3),
                (disc_hbm, disc, 4), (date_hbm, date, 5),
            )
        ]
        for load in loads[:3]:
            load.start()
        barrier = pltpu.get_barrier_semaphore()
        for there in across:
            pl.semaphore_signal(barrier, inc=1, device_id=there, device_id_type=MESH)
        for k, q in zip(path_steps, on_path):
            if k % 2 == 0:
                pl.semaphore_signal(barrier, inc=1, device_id={"path": q}, device_id_type=MESH)
        for y in range(1, n_path // 2):
            q = lax.rem(partner + 2 * y, n_path)
            pl.semaphore_signal(barrier, inc=1, device_id={"path": q}, device_id_type=MESH)
        for load in loads[3:]:
            load.start()

        def send(src, dst, send_sem, recv_sem, device):
            pltpu.make_async_remote_copy(
                src_ref=src, dst_ref=dst, send_sem=send_sem, recv_sem=recv_sem,
                device_id=device, device_id_type=MESH,
            ).start()

        arrive(where, in_sem.at[0])
        loc = where[1] - first_sent
        ids = jnp.where(
            (loc >= 0) & (loc < count), (loc // sub) * rows + where[0] * sub + lax.rem(loc, sub), -1
        )
        which = lax.broadcasted_iota(jnp.int32, (2 * rows, LANES), 0)
        places = lax.broadcasted_iota(jnp.int32, (rows, LANES), 0).astype(f32).astype(bf16)
        one, none = jnp.ones((rows, LANES), bf16), jnp.zeros((rows, LANES), bf16)
        local = [
            jnp.where((ids >= h * rows) & (ids < (h + 1) * rows), ids - h * rows, -1).astype(f32)
            for h in range(2)
        ]

        def picked(h, r):
            row = jnp.broadcast_to(local[h][r : r + 1, :], (16, LANES)).astype(bf16)
            return jnp.where(places == jnp.concatenate([row] * (rows // 16)), one, none)

        arrive(coef, in_sem.at[1])
        deep = tall // 2
        sums = 0.0
        for q in range(2):
            tile = jnp.concatenate(
                [
                    jnp.concatenate([picked(h, r) for r in range(q * deep, (q + 1) * deep)], axis=1)
                    for h in range(2)
                ]
            )
            sums = sums + jnp.dot(
                tile, coef[q * deep * LANES : (q + 1) * deep * LANES, :],
                preferred_element_type=f32,
            )
        part[...] = sums.astype(bf16).reshape(2, n_trade, sub, width)

        arrive(basis, in_sem.at[2])
        pl.semaphore_wait(barrier, n_trade + n_path - 2)
        for h in range(2):
            for j, (o, there) in enumerate(zip(others, across)):
                group = 0 if j < early else 1
                send(part.at[h, o], arrived.at[h, j], s1.at[0], r1.at[2 * h + group], there)
        send(basis, basis_other, sd.at[0], rd.at[0], {"path": partner})

        arrive(sets, in_sem.at[3])
        arrive(disc, in_sem.at[4])
        limit = level_step * jnp.sum(
            jnp.where(diagonal(count, n_set, first), sets[1].astype(f32), 0.0),
            axis=1, keepdims=True,
        )
        wanted = jnp.sum(
            jnp.where(diagonal(n_set, n_set, 0), sets[0].astype(f32), 0.0),
            axis=1, keepdims=True,
        )
        pick = lax.broadcasted_iota(jnp.int32, (n_set, factors), 1).astype(f32) == wanted
        pick = jnp.where(pick, 1.0, 0.0).astype(bf16)
        arrive(date, in_sem.at[5])
        dated[...] = jnp.dot(
            pick, date[...].astype(f32).astype(bf16), preferred_element_type=f32
        ).reshape(2, count, per_path)
        send(dated.at[1 - core], dated_other, sd.at[1], rd.at[1], {"path": partner})
        coef_t[...] = turned(coef[...])
        basis_t[0] = turned(basis[...])
        arrive(basis_other, rd.at[0])
        basis_t[1] = turned(basis_other[...])
        arrive(dated_other, rd.at[1])

        moment_of = lax.broadcasted_iota(jnp.int32, (sub, width), 1) // K
        for h in range(2):
            some_sets = slice(h * sub, (h + 1) * sub)
            total = jnp.zeros((sub, width), f32)
            for group, some in ((1, range(early, n_trade)), (0, range(early))):
                arrive(arrived.at[h, some.start : some.stop], r1.at[2 * h + group])
                for j in some:
                    total = total + arrived[h, j].astype(f32)
            stack = jnp.concatenate([jnp.where(moment_of == d, total, 0.0) for d in range(DATES)])
            high = stack.astype(bf16)
            low = (stack - high.astype(f32)).astype(bf16)
            grads = 0.0
            for i, (b_ref, when) in enumerate(
                ((basis, dated[core, some_sets]), (basis_other, dated_other[some_sets]))
            ):
                b = b_ref[...]
                netted = jnp.dot(high, b, preferred_element_type=f32) + jnp.dot(
                    low, b, preferred_element_type=f32
                )
                slopes = []
                for d in range(DATES):
                    x = netted[d * sub : (d + 1) * sub] - limit[some_sets]
                    e = jnp.exp(-jnp.abs(x))
                    inv = 1.0 / (1.0 + e)
                    sig = jnp.where(x >= 0, inv, e * inv)
                    factor_d = disc[0:1, d : d + 1] / (per_path * n_path)
                    weight = jnp.where(when == float(d), factor_d, 0.0)
                    excess[h, DATES * i + d] = x
                    weights[h, DATES * i + d] = weight
                    slopes.append(weight * sig)
                grads = grads + jnp.dot(
                    jnp.concatenate(slopes).astype(bf16), basis_t[i], preferred_element_type=f32
                )
            grad = jnp.zeros((sub, width), f32)
            for d in range(DATES):
                grad = grad + jnp.where(moment_of == d, grads[d * sub : (d + 1) * sub], 0.0)
            gmine[h] = grad.astype(bf16)
            for o in [0, 10, 6, 9, 11, 14, 2, 5, 7, 8, 13, 15, 1, 3, 4, 12]:
                there = {"trade": o, "path": partner}
                send(gmine.at[h], gall.at[h, me], s3.at[0], r3.at[h], there)
        cvas = []
        for h in range(2):
            cva = jnp.zeros((sub, per_path), f32)
            for i in range(2 * DATES):
                x = excess[h, i]
                plus = jnp.maximum(x, 0.0) + jnp.log1p(jnp.exp(-jnp.abs(x)))
                cva = cva + weights[h, i] * plus
            cvas.append(jnp.sum(cva, axis=1, keepdims=True))
        cva = jnp.concatenate(cvas)
        cva_mine[...] = jnp.sum(
            jnp.where(diagonal(count, n_set, first), cva, 0.0), axis=0, keepdims=True
        )
        for j, q in enumerate(on_path):
            send(cva_mine, cva_in.at[j], sc.at[0], rc.at[0], {"path": q})

        block = 2 * LANES
        for h in range(2):
            arrive(gall.at[h], r3.at[h])
            g = gall[h].reshape(rows, width)
            which = lax.broadcasted_iota(jnp.int32, (rows, LANES), 0) + h * rows
            for r in range(trades // block):
                dots = jnp.dot(
                    g, coef_t[:, r * block : (r + 1) * block], preferred_element_type=f32
                )
                for i in range(2):
                    at = 2 * r + i
                    hit = which == ids[at : at + 1, :]
                    share = jnp.sum(
                        jnp.where(hit, dots[:, i * LANES : (i + 1) * LANES], 0.0),
                        axis=0, keepdims=True,
                    )
                    if h == 0:
                        al_mine[at // 8, at % 8 : at % 8 + 1, :] = share
                    else:
                        al_mine[at // 8, at % 8 : at % 8 + 1, :] += share
                if h == 1 and (2 * r + 2) % 8 == 0:
                    i = (2 * r + 2) // 8 - 1
                    for j, q in enumerate(on_path):
                        send(al_mine.at[i], al_in.at[i, j], sa.at[0], ra.at[i], {"path": q})
        arrive(arrived, s1.at[0])
        arrive(arrived, s3.at[0])
        arrive(basis, sd.at[0])
        arrive(dated_other, sd.at[1])
        arrive(cva_in, sc.at[0])


        arrive(cva_in, rc.at[0])
        cva_total = cva_mine[...]
        for j in range(n_along):
            cva_total = cva_total + cva_in[j]
        cva_ref[...] = cva_total
        for i in range(tall // 8):
            arrive(al_in.at[i], ra.at[i])
            total_alloc = al_mine[i]
            for j in range(n_along):
                total_alloc = total_alloc + al_in[i, j]
            alloc_ref[i * 8 : (i + 1) * 8] = total_alloc
        arrive(al_in, sa.at[0])

    return kernel


def write_out(alloc, cva, alloc_out, cva_out, sem):
    copies = [
        pltpu.make_async_copy(src, dst, sem.at[i])
        for i, (src, dst) in enumerate(((alloc, alloc_out), (cva, cva_out)))
    ]
    for copy in copies:
        copy.start()
    for copy in copies:
        copy.wait()


def solution(mesh):
    n_trade, n_path = mesh.shape["trade"], mesh.shape["path"]
    side = 4

    def on_device(
        coefficients, path_basis, trade_owner, trade_slot, set_factor, set_level, default_date,
        discount,
    ):
        trades, width = coefficients.shape
        n_set = set_factor.shape[0]
        factors, per_path = default_date.shape
        tall = trades // LANES
        half = n_set // 2
        bf16, f32, i32 = jnp.bfloat16, jnp.float32, jnp.int32
        dma = pltpu.SemaphoreType.DMA
        alloc, cva = pl.pallas_call(
            make_kernel(n_trade, n_path, side, n_set, trades, per_path, factors),
            out_shape=(pltpu.VMEM((tall, LANES), f32), pltpu.VMEM((1, n_set), f32)),
            in_specs=[pl.BlockSpec(memory_space=pl.ANY)] * 8,
            out_specs=(
                pl.BlockSpec(memory_space=pltpu.VMEM),
                pl.BlockSpec(memory_space=pltpu.VMEM),
            ),
            scratch_shapes=[
                pltpu.VMEM((trades, width), bf16),
                pltpu.VMEM((width, trades), bf16),
                pltpu.VMEM((width, per_path), bf16),
                pltpu.VMEM((width, per_path), bf16),
                pltpu.VMEM((2, per_path, width), bf16),
                pltpu.VMEM((2, tall, LANES), i32),
                pltpu.VMEM((2, 1, n_set), i32),
                pltpu.VMEM((factors, per_path), i32),
                pltpu.VMEM((1, DATES), f32),
                pltpu.VMEM((n_trade * half, trades), bf16),
                pltpu.VMEM((2, half, per_path), f32),
                pltpu.VMEM((half, per_path), f32),
                pltpu.VMEM((2, 2 * DATES, half // 2, per_path), f32),
                pltpu.VMEM((2, 2 * DATES, half // 2, per_path), f32),
                pltpu.VMEM((1, n_set), f32),
                pltpu.VMEM((n_path - 1, 1, n_set), f32),
                pltpu.VMEM((tall // 8, 8, LANES), f32),
                pltpu.VMEM((tall // 8, n_path - 1, 8, LANES), f32),
                pltpu.VMEM((2, n_trade, half // 2, width), bf16),
                pltpu.VMEM((2, n_trade, half // 2, width), bf16),
                pltpu.VMEM((2, half // 2, width), bf16),
                pltpu.VMEM((2, n_trade, half // 2, width), bf16),
                dma((6,)),
                dma((1,)),
                dma((4,)),
                dma((2,)),
                dma((2,)),
                dma((1,)),
                dma((2,)),
                dma((1,)),
                dma((1,)),
                dma((1,)),
                dma((2,)),
            ],
            compiler_params=pltpu.CompilerParams(collective_id=0, has_side_effects=True),
        )(
            coefficients,
            path_basis,
            trade_owner.reshape(tall, LANES),
            trade_slot.reshape(tall, LANES),
            set_factor.reshape(1, n_set),
            set_level.reshape(1, n_set),
            default_date,
            discount.reshape(1, DATES),
        )
        alloc, cva = pl.pallas_call(
            write_out,
            out_shape=(
                jax.ShapeDtypeStruct((tall, LANES), f32),
                jax.ShapeDtypeStruct((1, n_set), f32),
            ),
            in_specs=[pl.BlockSpec(memory_space=pltpu.VMEM)] * 2,
            out_specs=(
                pl.BlockSpec(memory_space=pltpu.HBM),
                pl.BlockSpec(memory_space=pltpu.HBM),
            ),
            scratch_shapes=[dma((2,))],
            compiler_params=pltpu.CompilerParams(vmem_limit_bytes=1 << 20),
        )(alloc, cva)
        return alloc.reshape(trades), cva.reshape(n_set)

    return jax.shard_map(
        on_device,
        mesh=mesh,
        in_specs=(
            P("trade", None),
            P(None, "path"),
            P("trade", None),
            P("trade"),
            P("trade"),
            P("trade"),
            P(None, "path"),
            P(),
        ),
        out_specs=(P("trade"), P("trade")),
        check_vma=False,
    )
```

```python
import jax
import jax.numpy as jnp
from jax import lax
from jax.experimental import pallas as pl
from jax.experimental.pallas import tpu as pltpu
from jax.sharding import PartitionSpec as P

MESH = pl.DeviceIdType.MESH
K = 64
DATES = 4
LANES = 128
level_step = 1.5


def grid_offsets(side):
    def far(step):
        return min(step, side - step)

    offsets = [(a, b) for a in range(side) for b in range(side)]
    return sorted(offsets, key=lambda o: (-(far(o[0]) + far(o[1])), (o[0] + 2 * o[1]) % 4, o[0]))


def diagonal(rows, columns, first):
    at = lax.broadcasted_iota(jnp.int32, (rows, columns), 0) + first
    return at == lax.broadcasted_iota(jnp.int32, (rows, columns), 1)


def arrive(ref, sem):
    pltpu.make_async_copy(ref, ref, sem).wait()


def turned(x):
    size = x.shape[1]
    ones = jnp.where(diagonal(size, size, 0), 1.0, 0.0).astype(x.dtype)
    return lax.dot_general(
        ones, x, (((1,), (1,)), ((), ())), preferred_element_type=jnp.float32
    ).astype(x.dtype)


def make_kernel(n_trade, n_path, side, n_set, trades, per_path, factors):
    offsets = grid_offsets(side)
    n_along = n_path - 1
    count = n_set // 2
    sub = count // 2
    rows = n_trade * sub
    width = DATES * K
    path_steps = sorted(range(1, n_path), key=lambda k: (2, 4, 3, 5, 6, 7, 1).index(k))
    early = n_trade // 2 + 1
    tall = trades // LANES
    f32, bf16 = jnp.float32, jnp.bfloat16

    def kernel(
        coef_hbm, basis_hbm, owner_hbm, slot_hbm, factor_hbm, level_hbm, date_hbm, disc_hbm,
        alloc_ref, cva_ref,
        coef, coef_t, basis, basis_other, basis_t, where, sets, date, disc, onehot, dated, dated_other, excess, weights,
        cva_mine, cva_in, al_mine, al_in, part, arrived, gmine, gall,
        in_sem, s1, r1, sd, rd, s3, r3, sc, rc, sa, ra,
    ):
        me = lax.axis_index("trade")
        lane = lax.axis_index("path")
        core = lax.rem(lane, 2)
        partner = lane + 1 - 2 * core
        me_a, me_b = me // side, lax.rem(me, side)
        others = [
            lax.rem(me_a + a, side) * side + lax.rem(me_b + b, side) for a, b in offsets
        ]
        on_path = [lax.rem(lane + k, n_path) for k in path_steps]

        across = [{"trade": o, "path": partner} for o in others]
        first, first_sent = count * core, count * (1 - core)

        loads = [
            pltpu.make_async_copy(src, dst, in_sem.at[i])
            for src, dst, i in (
                (owner_hbm, where.at[0], 0), (slot_hbm, where.at[1], 0), (coef_hbm, coef, 1),
                (basis_hbm, basis, 2), (factor_hbm, sets.at[0], 3), (level_hbm, sets.at[1], 3),
                (disc_hbm, disc, 4), (date_hbm, date, 5),
            )
        ]
        for load in loads[:3]:
            load.start()
        barrier = pltpu.get_barrier_semaphore()
        for there in across:
            pl.semaphore_signal(barrier, inc=1, device_id=there, device_id_type=MESH)
        for k, q in zip(path_steps, on_path):
            if k % 2 == 0:
                pl.semaphore_signal(barrier, inc=1, device_id={"path": q}, device_id_type=MESH)
        for y in range(1, n_path // 2):
            q = lax.rem(partner + 2 * y, n_path)
            pl.semaphore_signal(barrier, inc=1, device_id={"path": q}, device_id_type=MESH)
        for load in loads[3:]:
            load.start()

        def send(src, dst, send_sem, recv_sem, device):
            pltpu.make_async_remote_copy(
                src_ref=src, dst_ref=dst, send_sem=send_sem, recv_sem=recv_sem,
                device_id=device, device_id_type=MESH,
            ).start()

        arrive(where, in_sem.at[0])
        loc = where[1] - first_sent
        ids = jnp.where(
            (loc >= 0) & (loc < count), (loc // sub) * rows + where[0] * sub + lax.rem(loc, sub), -1
        )
        which = lax.broadcasted_iota(jnp.int32, (2 * rows, LANES), 0)
        places = lax.broadcasted_iota(jnp.int32, (rows, LANES), 0).astype(f32).astype(bf16)
        one, none = jnp.ones((rows, LANES), bf16), jnp.zeros((rows, LANES), bf16)
        local = [
            jnp.where((ids >= h * rows) & (ids < (h + 1) * rows), ids - h * rows, -1).astype(f32)
            for h in range(2)
        ]

        def picked(h, r):
            row = jnp.broadcast_to(local[h][r : r + 1, :], (16, LANES)).astype(bf16)
            return jnp.where(places == jnp.concatenate([row] * (rows // 16)), one, none)

        arrive(coef, in_sem.at[1])
        deep = tall // 2
        sums = 0.0
        for q in range(2):
            tile = jnp.concatenate(
                [
                    jnp.concatenate([picked(h, r) for r in range(q * deep, (q + 1) * deep)], axis=1)
                    for h in range(2)
                ]
            )
            sums = sums + jnp.dot(
                tile, coef[q * deep * LANES : (q + 1) * deep * LANES, :],
                preferred_element_type=f32,
            )
        part[...] = sums.astype(bf16).reshape(2, n_trade, sub, width)

        arrive(basis, in_sem.at[2])
        pl.semaphore_wait(barrier, n_trade + n_path - 2)
        for h in range(2):
            for j, (o, there) in enumerate(zip(others, across)):
                group = 0
                send(part.at[h, o], arrived.at[h, j], s1.at[0], r1.at[h], there)
        send(basis, basis_other, sd.at[0], rd.at[0], {"path": partner})

        arrive(sets, in_sem.at[3])
        arrive(disc, in_sem.at[4])
        limit = level_step * jnp.sum(
            jnp.where(diagonal(count, n_set, first), sets[1].astype(f32), 0.0),
            axis=1, keepdims=True,
        )
        wanted = jnp.sum(
            jnp.where(diagonal(n_set, n_set, 0), sets[0].astype(f32), 0.0),
            axis=1, keepdims=True,
        )
        pick = lax.broadcasted_iota(jnp.int32, (n_set, factors), 1).astype(f32) == wanted
        pick = jnp.where(pick, 1.0, 0.0).astype(bf16)
        arrive(date, in_sem.at[5])
        dated[...] = jnp.dot(
            pick, date[...].astype(f32).astype(bf16), preferred_element_type=f32
        ).reshape(2, count, per_path)
        send(dated.at[1 - core], dated_other, sd.at[1], rd.at[1], {"path": partner})
        coef_t[...] = turned(coef[...])
        basis_t[0] = turned(basis[...])
        arrive(basis_other, rd.at[0])
        basis_t[1] = turned(basis_other[...])
        arrive(dated_other, rd.at[1])

        moment_of = lax.broadcasted_iota(jnp.int32, (sub, width), 1) // K
        for h in range(2):
            some_sets = slice(h * sub, (h + 1) * sub)
            total = jnp.zeros((sub, width), f32)
            for group, some in ((0, range(n_trade)),):
                arrive(arrived.at[h, some.start : some.stop], r1.at[h])
                for j in some:
                    total = total + arrived[h, j].astype(f32)
            high = total.astype(bf16)
            low = (total - high.astype(f32)).astype(bf16)
            nothing = jnp.zeros_like(high)
            stack = jnp.concatenate(
                [jnp.where(moment_of == d, x, nothing) for x in (high, low) for d in range(DATES)]
            )
            grads = 0.0
            for i, (b_ref, when) in enumerate(
                ((basis, dated[core, some_sets]), (basis_other, dated_other[some_sets]))
            ):
                b = b_ref[...]
                netted = jnp.dot(stack, b, preferred_element_type=f32)
                netted = netted[: DATES * sub] + netted[DATES * sub :]
                slopes = []
                for d in range(DATES):
                    x = netted[d * sub : (d + 1) * sub] - limit[some_sets]
                    e = jnp.exp(-jnp.abs(x))
                    inv = 1.0 / (1.0 + e)
                    sig = jnp.where(x >= 0, inv, e * inv)
                    factor_d = disc[0:1, d : d + 1] / (per_path * n_path)
                    weight = jnp.where(when == float(d), factor_d, 0.0)
                    excess[h, DATES * i + d] = x
                    weights[h, DATES * i + d] = weight
                    slopes.append(weight * sig)
                grads = grads + jnp.dot(
                    jnp.concatenate(slopes).astype(bf16), basis_t[i], preferred_element_type=f32
                )
            grad = jnp.zeros((sub, width), f32)
            for d in range(DATES):
                grad = grad + jnp.where(moment_of == d, grads[d * sub : (d + 1) * sub], 0.0)
            gmine[h] = grad.astype(bf16)
            for o in [0, 10, 6, 9, 11, 14, 2, 5, 7, 8, 13, 15, 1, 3, 4, 12]:
                there = {"trade": o, "path": partner}
                send(gmine.at[h], gall.at[h, me], s3.at[0], r3.at[h], there)
        cvas = []
        for h in range(2):
            cva = jnp.zeros((sub, per_path), f32)
            for i in range(2 * DATES):
                x = excess[h, i]
                plus = jnp.maximum(x, 0.0) + jnp.log1p(jnp.exp(-jnp.abs(x)))
                cva = cva + weights[h, i] * plus
            cvas.append(jnp.sum(cva, axis=1, keepdims=True))
        cva = jnp.concatenate(cvas)
        cva_mine[...] = jnp.sum(
            jnp.where(diagonal(count, n_set, first), cva, 0.0), axis=0, keepdims=True
        )
        for j, q in enumerate(on_path):
            send(cva_mine, cva_in.at[j], sc.at[0], rc.at[0], {"path": q})

        block = 2 * LANES
        for h in range(2):
            arrive(gall.at[h], r3.at[h])
            g = gall[h].reshape(rows, width)
            which = lax.broadcasted_iota(jnp.int32, (rows, LANES), 0) + h * rows
            for r in range(trades // block):
                dots = jnp.dot(
                    g, coef_t[:, r * block : (r + 1) * block], preferred_element_type=f32
                )
                for i in range(2):
                    at = 2 * r + i
                    hit = which == ids[at : at + 1, :]
                    share = jnp.sum(
                        jnp.where(hit, dots[:, i * LANES : (i + 1) * LANES], 0.0),
                        axis=0, keepdims=True,
                    )
                    if h == 0:
                        al_mine[at // 8, at % 8 : at % 8 + 1, :] = share
                    else:
                        al_mine[at // 8, at % 8 : at % 8 + 1, :] += share
                if h == 1 and (2 * r + 2) % 8 == 0:
                    i = (2 * r + 2) // 8 - 1
                    for j, q in enumerate(on_path):
                        send(al_mine.at[i], al_in.at[i, j], sa.at[0], ra.at[i], {"path": q})
        arrive(arrived, s1.at[0])
        arrive(arrived, s3.at[0])
        arrive(basis, sd.at[0])
        arrive(dated_other, sd.at[1])
        arrive(cva_in, sc.at[0])


        arrive(cva_in, rc.at[0])
        cva_total = cva_mine[...]
        for j in range(n_along):
            cva_total = cva_total + cva_in[j]
        cva_ref[...] = cva_total
        for i in range(tall // 8):
            arrive(al_in.at[i], ra.at[i])
            total_alloc = al_mine[i]
            for j in range(n_along):
                total_alloc = total_alloc + al_in[i, j]
            alloc_ref[i * 8 : (i + 1) * 8] = total_alloc
        arrive(al_in, sa.at[0])

    return kernel


def write_out(alloc, cva, alloc_out, cva_out, sem):
    copies = [
        pltpu.make_async_copy(src, dst, sem.at[i])
        for i, (src, dst) in enumerate(((alloc, alloc_out), (cva, cva_out)))
    ]
    for copy in copies:
        copy.start()
    for copy in copies:
        copy.wait()


def solution(mesh):
    n_trade, n_path = mesh.shape["trade"], mesh.shape["path"]
    side = 4

    def on_device(
        coefficients, path_basis, trade_owner, trade_slot, set_factor, set_level, default_date,
        discount,
    ):
        trades, width = coefficients.shape
        n_set = set_factor.shape[0]
        factors, per_path = default_date.shape
        tall = trades // LANES
        half = n_set // 2
        bf16, f32, i32 = jnp.bfloat16, jnp.float32, jnp.int32
        dma = pltpu.SemaphoreType.DMA
        alloc, cva = pl.pallas_call(
            make_kernel(n_trade, n_path, side, n_set, trades, per_path, factors),
            out_shape=(pltpu.VMEM((tall, LANES), f32), pltpu.VMEM((1, n_set), f32)),
            in_specs=[pl.BlockSpec(memory_space=pl.ANY)] * 8,
            out_specs=(
                pl.BlockSpec(memory_space=pltpu.VMEM),
                pl.BlockSpec(memory_space=pltpu.VMEM),
            ),
            scratch_shapes=[
                pltpu.VMEM((trades, width), bf16),
                pltpu.VMEM((width, trades), bf16),
                pltpu.VMEM((width, per_path), bf16),
                pltpu.VMEM((width, per_path), bf16),
                pltpu.VMEM((2, per_path, width), bf16),
                pltpu.VMEM((2, tall, LANES), i32),
                pltpu.VMEM((2, 1, n_set), i32),
                pltpu.VMEM((factors, per_path), i32),
                pltpu.VMEM((1, DATES), f32),
                pltpu.VMEM((n_trade * half, trades), bf16),
                pltpu.VMEM((2, half, per_path), f32),
                pltpu.VMEM((half, per_path), f32),
                pltpu.VMEM((2, 2 * DATES, half // 2, per_path), f32),
                pltpu.VMEM((2, 2 * DATES, half // 2, per_path), f32),
                pltpu.VMEM((1, n_set), f32),
                pltpu.VMEM((n_path - 1, 1, n_set), f32),
                pltpu.VMEM((tall // 8, 8, LANES), f32),
                pltpu.VMEM((tall // 8, n_path - 1, 8, LANES), f32),
                pltpu.VMEM((2, n_trade, half // 2, width), bf16),
                pltpu.VMEM((2, n_trade, half // 2, width), bf16),
                pltpu.VMEM((2, half // 2, width), bf16),
                pltpu.VMEM((2, n_trade, half // 2, width), bf16),
                dma((6,)),
                dma((1,)),
                dma((2,)),
                dma((2,)),
                dma((2,)),
                dma((1,)),
                dma((2,)),
                dma((1,)),
                dma((1,)),
                dma((1,)),
                dma((2,)),
            ],
            compiler_params=pltpu.CompilerParams(collective_id=0, has_side_effects=True),
        )(
            coefficients,
            path_basis,
            trade_owner.reshape(tall, LANES),
            trade_slot.reshape(tall, LANES),
            set_factor.reshape(1, n_set),
            set_level.reshape(1, n_set),
            default_date,
            discount.reshape(1, DATES),
        )
        alloc, cva = pl.pallas_call(
            write_out,
            out_shape=(
                jax.ShapeDtypeStruct((tall, LANES), f32),
                jax.ShapeDtypeStruct((1, n_set), f32),
            ),
            in_specs=[pl.BlockSpec(memory_space=pltpu.VMEM)] * 2,
            out_specs=(
                pl.BlockSpec(memory_space=pltpu.HBM),
                pl.BlockSpec(memory_space=pltpu.HBM),
            ),
            scratch_shapes=[dma((2,))],
            compiler_params=pltpu.CompilerParams(vmem_limit_bytes=1 << 20),
        )(alloc, cva)
        return alloc.reshape(trades), cva.reshape(n_set)

    return jax.shard_map(
        on_device,
        mesh=mesh,
        in_specs=(
            P("trade", None),
            P(None, "path"),
            P("trade", None),
            P("trade"),
            P("trade"),
            P("trade"),
            P(None, "path"),
            P(),
        ),
        out_specs=(P("trade"), P("trade")),
        check_vma=False,
    )
```

```python
import jax
import jax.numpy as jnp
from jax import lax
from jax.experimental import pallas as pl
from jax.experimental.pallas import tpu as pltpu
from jax.sharding import PartitionSpec as P

MESH = pl.DeviceIdType.MESH
K = 64
DATES = 4
LANES = 128
level_step = 1.5


def grid_offsets(side):
    def far(step):
        return min(step, side - step)

    offsets = [(a, b) for a in range(side) for b in range(side)]
    return sorted(offsets, key=lambda o: (-(far(o[0]) + far(o[1])), (o[0] + o[1]) % 4, -o[0]))


def diagonal(rows, columns, first):
    at = lax.broadcasted_iota(jnp.int32, (rows, columns), 0) + first
    return at == lax.broadcasted_iota(jnp.int32, (rows, columns), 1)


def arrive(ref, sem):
    pltpu.make_async_copy(ref, ref, sem).wait()


def turned(x):
    size = x.shape[1]
    ones = jnp.where(diagonal(size, size, 0), 1.0, 0.0).astype(x.dtype)
    return lax.dot_general(
        ones, x, (((1,), (1,)), ((), ())), preferred_element_type=jnp.float32
    ).astype(x.dtype)


def make_kernel(n_trade, n_path, side, n_set, trades, per_path, factors):
    offsets = grid_offsets(side)
    n_along = n_path - 1
    count = n_set // 2
    sub = count // 2
    rows = n_trade * sub
    width = DATES * K
    path_steps = sorted(range(1, n_path), key=lambda k: (2, 4, 3, 5, 6, 7, 1).index(k))
    early = n_trade // 2 + 1
    tall = trades // LANES
    f32, bf16 = jnp.float32, jnp.bfloat16

    def kernel(
        coef_hbm, basis_hbm, owner_hbm, slot_hbm, factor_hbm, level_hbm, date_hbm, disc_hbm,
        alloc_ref, cva_ref,
        coef, coef_t, basis, basis_other, basis_t, where, sets, date, disc, dated, dated_other, excess, weights,
        cva_mine, cva_in, al_mine, al_in, part, arrived, gmine, gall,
        in_sem, s1, r1, sd, rd, s3, r3, sc, rc, sa, ra,
    ):
        me = lax.axis_index("trade")
        lane = lax.axis_index("path")
        core = lax.rem(lane, 2)
        partner = lane + 1 - 2 * core
        me_a, me_b = me // side, lax.rem(me, side)
        others = [
            lax.rem(me_a + a, side) * side + lax.rem(me_b + b, side) for a, b in offsets
        ]
        on_path = [lax.rem(lane + k, n_path) for k in path_steps]

        across = [{"trade": o, "path": partner} for o in others]
        first, first_sent = count * core, count * (1 - core)

        loads = [
            pltpu.make_async_copy(src, dst, in_sem.at[i])
            for src, dst, i in (
                (owner_hbm, where.at[0], 0), (slot_hbm, where.at[1], 0), (coef_hbm, coef, 1),
                (basis_hbm, basis, 2), (factor_hbm, sets.at[0], 3), (level_hbm, sets.at[1], 3),
                (disc_hbm, disc, 4), (date_hbm, date, 5),
            )
        ]
        for load in loads[:3]:
            load.start()
        barrier = pltpu.get_barrier_semaphore()
        for there in across:
            pl.semaphore_signal(barrier, inc=1, device_id=there, device_id_type=MESH)
        for k, q in zip(path_steps, on_path):
            if k % 2 == 0:
                pl.semaphore_signal(barrier, inc=1, device_id={"path": q}, device_id_type=MESH)
        for y in range(1, n_path // 2):
            q = lax.rem(partner + 2 * y, n_path)
            pl.semaphore_signal(barrier, inc=1, device_id={"path": q}, device_id_type=MESH)
        for load in loads[3:]:
            load.start()

        def send(src, dst, send_sem, recv_sem, device):
            pltpu.make_async_remote_copy(
                src_ref=src, dst_ref=dst, send_sem=send_sem, recv_sem=recv_sem,
                device_id=device, device_id_type=MESH,
            ).start()

        arrive(where, in_sem.at[0])
        loc = where[1] - first_sent
        ids = jnp.where(
            (loc >= 0) & (loc < count), (loc // sub) * rows + where[0] * sub + lax.rem(loc, sub), -1
        )
        which = lax.broadcasted_iota(jnp.int32, (2 * rows, LANES), 0)
        places = lax.broadcasted_iota(jnp.int32, (rows, LANES), 0).astype(f32).astype(bf16)
        one, none = jnp.ones((rows, LANES), bf16), jnp.zeros((rows, LANES), bf16)
        local = [
            jnp.where((ids >= h * rows) & (ids < (h + 1) * rows), ids - h * rows, -1).astype(f32)
            for h in range(2)
        ]

        def picked(h, r):
            row = jnp.broadcast_to(local[h][r : r + 1, :], (16, LANES)).astype(bf16)
            return jnp.where(places == jnp.concatenate([row] * (rows // 16)), one, none)

        arrive(coef, in_sem.at[1])
        deep = tall // 2
        sums = 0.0
        for q in range(2):
            tile = jnp.concatenate(
                [
                    jnp.concatenate([picked(h, r) for r in range(q * deep, (q + 1) * deep)], axis=1)
                    for h in range(2)
                ]
            )
            sums = sums + jnp.dot(
                tile, coef[q * deep * LANES : (q + 1) * deep * LANES, :],
                preferred_element_type=f32,
            )
        part[...] = sums.astype(bf16).reshape(2, n_trade, sub, width)

        arrive(basis, in_sem.at[2])
        pl.semaphore_wait(barrier, n_trade + n_path - 2)
        for h in range(2):
            for j, (o, there) in enumerate(zip(others, across)):
                group = 0
                send(part.at[h, o], arrived.at[h, j], s1.at[0], r1.at[h], there)
        send(basis, basis_other, sd.at[0], rd.at[0], {"path": partner})

        arrive(sets, in_sem.at[3])
        arrive(disc, in_sem.at[4])
        limit = level_step * jnp.sum(
            jnp.where(diagonal(count, n_set, first), sets[1].astype(f32), 0.0),
            axis=1, keepdims=True,
        )
        wanted = jnp.sum(
            jnp.where(diagonal(n_set, n_set, 0), sets[0].astype(f32), 0.0),
            axis=1, keepdims=True,
        )
        pick = lax.broadcasted_iota(jnp.int32, (n_set, factors), 1).astype(f32) == wanted
        pick = jnp.where(pick, 1.0, 0.0).astype(bf16)
        arrive(date, in_sem.at[5])
        dated[...] = jnp.dot(
            pick, date[...].astype(f32).astype(bf16), preferred_element_type=f32
        ).reshape(2, count, per_path)
        send(dated.at[1 - core], dated_other, sd.at[1], rd.at[1], {"path": partner})
        coef_t[...] = turned(coef[...])
        basis_t[0] = turned(basis[...])
        arrive(basis_other, rd.at[0])
        basis_t[1] = turned(basis_other[...])
        arrive(dated_other, rd.at[1])

        moment_of = lax.broadcasted_iota(jnp.int32, (sub, width), 1) // K
        for h in range(2):
            some_sets = slice(h * sub, (h + 1) * sub)
            total = jnp.zeros((sub, width), f32)
            for group, some in ((0, range(n_trade)),):
                arrive(arrived.at[h, some.start : some.stop], r1.at[h])
                for j in some:
                    total = total + arrived[h, j].astype(f32)
            high = total.astype(bf16)
            low = (total - high.astype(f32)).astype(bf16)
            nothing = jnp.zeros_like(high)
            stack = jnp.concatenate(
                [jnp.where(moment_of == d, x, nothing) for x in (high, low) for d in range(DATES)]
            )
            grads = 0.0
            for i, (b_ref, when) in enumerate(
                ((basis, dated[core, some_sets]), (basis_other, dated_other[some_sets]))
            ):
                b = b_ref[...]
                netted = jnp.dot(stack, b, preferred_element_type=f32)
                netted = netted[: DATES * sub] + netted[DATES * sub :]
                slopes = []
                for d in range(DATES):
                    x = netted[d * sub : (d + 1) * sub] - limit[some_sets]
                    e = jnp.exp(-jnp.abs(x))
                    inv = 1.0 / (1.0 + e)
                    sig = jnp.where(x >= 0, inv, e * inv)
                    factor_d = disc[0:1, d : d + 1] / (per_path * n_path)
                    weight = jnp.where(when == float(d), factor_d, 0.0)
                    excess[h, DATES * i + d] = x
                    weights[h, DATES * i + d] = weight
                    slopes.append(weight * sig)
                grads = grads + jnp.dot(
                    jnp.concatenate(slopes).astype(bf16), basis_t[i], preferred_element_type=f32
                )
            grad = jnp.zeros((sub, width), f32)
            for d in range(DATES):
                grad = grad + jnp.where(moment_of == d, grads[d * sub : (d + 1) * sub], 0.0)
            gmine[h] = grad.astype(bf16)
            for o in [0, 10, 6, 9, 11, 14, 2, 5, 7, 8, 13, 15, 1, 3, 4, 12]:
                there = {"trade": o, "path": partner}
                send(gmine.at[h], gall.at[h, me], s3.at[0], r3.at[h], there)
        cvas = []
        for h in range(2):
            cva = jnp.zeros((sub, per_path), f32)
            for i in range(2 * DATES):
                x = excess[h, i]
                plus = jnp.maximum(x, 0.0) + jnp.log1p(jnp.exp(-jnp.abs(x)))
                cva = cva + weights[h, i] * plus
            cvas.append(jnp.sum(cva, axis=1, keepdims=True))
        cva = jnp.concatenate(cvas)
        cva_mine[...] = jnp.sum(
            jnp.where(diagonal(count, n_set, first), cva, 0.0), axis=0, keepdims=True
        )
        for j, q in enumerate(on_path):
            send(cva_mine, cva_in.at[j], sc.at[0], rc.at[0], {"path": q})

        block = 2 * LANES
        for h in range(2):
            arrive(gall.at[h], r3.at[h])
            g = gall[h].reshape(rows, width)
            which = lax.broadcasted_iota(jnp.int32, (rows, LANES), 0) + h * rows
            for r in range(trades // block):
                dots = jnp.dot(
                    g, coef_t[:, r * block : (r + 1) * block], preferred_element_type=f32
                )
                for i in range(2):
                    at = 2 * r + i
                    hit = which == ids[at : at + 1, :]
                    share = jnp.sum(
                        jnp.where(hit, dots[:, i * LANES : (i + 1) * LANES], 0.0),
                        axis=0, keepdims=True,
                    )
                    if h == 0:
                        al_mine[at // 8, at % 8 : at % 8 + 1, :] = share
                    else:
                        al_mine[at // 8, at % 8 : at % 8 + 1, :] += share
                if h == 1 and (2 * r + 2) % 8 == 0:
                    i = (2 * r + 2) // 8 - 1
                    for j, q in enumerate(on_path):
                        send(al_mine.at[i], al_in.at[i, j], sa.at[0], ra.at[i], {"path": q})
        arrive(arrived, s1.at[0])
        arrive(arrived, s3.at[0])
        arrive(basis, sd.at[0])
        arrive(dated_other, sd.at[1])
        arrive(cva_in, sc.at[0])


        arrive(cva_in, rc.at[0])
        cva_total = cva_mine[...]
        for j in range(n_along):
            cva_total = cva_total + cva_in[j]
        cva_ref[...] = cva_total
        for i in range(tall // 8):
            arrive(al_in.at[i], ra.at[i])
            total_alloc = al_mine[i]
            for j in range(n_along):
                total_alloc = total_alloc + al_in[i, j]
            alloc_ref[i * 8 : (i + 1) * 8] = total_alloc
        arrive(al_in, sa.at[0])

    return kernel


def write_out(alloc, cva, alloc_out, cva_out, sem):
    copies = [
        pltpu.make_async_copy(src, dst, sem.at[i])
        for i, (src, dst) in enumerate(((alloc, alloc_out), (cva, cva_out)))
    ]
    for copy in copies:
        copy.start()
    for copy in copies:
        copy.wait()


def solution(mesh):
    n_trade, n_path = mesh.shape["trade"], mesh.shape["path"]
    side = 4

    def on_device(
        coefficients, path_basis, trade_owner, trade_slot, set_factor, set_level, default_date,
        discount,
    ):
        trades, width = coefficients.shape
        n_set = set_factor.shape[0]
        factors, per_path = default_date.shape
        tall = trades // LANES
        half = n_set // 2
        bf16, f32, i32 = jnp.bfloat16, jnp.float32, jnp.int32
        dma = pltpu.SemaphoreType.DMA
        alloc, cva = pl.pallas_call(
            make_kernel(n_trade, n_path, side, n_set, trades, per_path, factors),
            out_shape=(pltpu.VMEM((tall, LANES), f32), pltpu.VMEM((1, n_set), f32)),
            in_specs=[pl.BlockSpec(memory_space=pl.ANY)] * 8,
            out_specs=(
                pl.BlockSpec(memory_space=pltpu.VMEM),
                pl.BlockSpec(memory_space=pltpu.VMEM),
            ),
            scratch_shapes=[
                pltpu.VMEM((trades, width), bf16),
                pltpu.VMEM((width, trades), bf16),
                pltpu.VMEM((width, per_path), bf16),
                pltpu.VMEM((width, per_path), bf16),
                pltpu.VMEM((2, per_path, width), bf16),
                pltpu.VMEM((2, tall, LANES), i32),
                pltpu.VMEM((2, 1, n_set), i32),
                pltpu.VMEM((factors, per_path), i32),
                pltpu.VMEM((1, DATES), f32),
                pltpu.VMEM((2, half, per_path), f32),
                pltpu.VMEM((half, per_path), f32),
                pltpu.VMEM((2, 2 * DATES, half // 2, per_path), f32),
                pltpu.VMEM((2, 2 * DATES, half // 2, per_path), f32),
                pltpu.VMEM((1, n_set), f32),
                pltpu.VMEM((n_path - 1, 1, n_set), f32),
                pltpu.VMEM((tall // 8, 8, LANES), f32),
                pltpu.VMEM((tall // 8, n_path - 1, 8, LANES), f32),
                pltpu.VMEM((2, n_trade, half // 2, width), bf16),
                pltpu.VMEM((2, n_trade, half // 2, width), bf16),
                pltpu.VMEM((2, half // 2, width), bf16),
                pltpu.VMEM((2, n_trade, half // 2, width), bf16),
                dma((6,)),
                dma((1,)),
                dma((2,)),
                dma((2,)),
                dma((2,)),
                dma((1,)),
                dma((2,)),
                dma((1,)),
                dma((1,)),
                dma((1,)),
                dma((2,)),
            ],
            compiler_params=pltpu.CompilerParams(collective_id=0, has_side_effects=True),
        )(
            coefficients,
            path_basis,
            trade_owner.reshape(tall, LANES),
            trade_slot.reshape(tall, LANES),
            set_factor.reshape(1, n_set),
            set_level.reshape(1, n_set),
            default_date,
            discount.reshape(1, DATES),
        )
        alloc, cva = pl.pallas_call(
            write_out,
            out_shape=(
                jax.ShapeDtypeStruct((tall, LANES), f32),
                jax.ShapeDtypeStruct((1, n_set), f32),
            ),
            in_specs=[pl.BlockSpec(memory_space=pltpu.VMEM)] * 2,
            out_specs=(
                pl.BlockSpec(memory_space=pltpu.HBM),
                pl.BlockSpec(memory_space=pltpu.HBM),
            ),
            scratch_shapes=[dma((2,))],
            compiler_params=pltpu.CompilerParams(vmem_limit_bytes=1 << 20),
        )(alloc, cva)
        return alloc.reshape(trades), cva.reshape(n_set)

    return jax.shard_map(
        on_device,
        mesh=mesh,
        in_specs=(
            P("trade", None),
            P(None, "path"),
            P("trade", None),
            P("trade"),
            P("trade"),
            P("trade"),
            P(None, "path"),
            P(),
        ),
        out_specs=(P("trade"), P("trade")),
        check_vma=False,
    )
```

```python
import jax
import jax.numpy as jnp
from jax import lax
from jax.experimental import pallas as pl
from jax.experimental.pallas import tpu as pltpu
from jax.sharding import PartitionSpec as P

MESH = pl.DeviceIdType.MESH
K = 64
DATES = 4
LANES = 128
level_step = 1.5


def grid_offsets(side):
    def far(step):
        return min(step, side - step)

    offsets = [(a, b) for a in range(side) for b in range(side)]
    return sorted(offsets, key=lambda o: (-(far(o[0]) + far(o[1])), (o[0] + 2 * o[1]) % 4, o[0]))


def diagonal(rows, columns, first):
    at = lax.broadcasted_iota(jnp.int32, (rows, columns), 0) + first
    return at == lax.broadcasted_iota(jnp.int32, (rows, columns), 1)


def arrive(ref, sem):
    pltpu.make_async_copy(ref, ref, sem).wait()


def turned(x):
    size = x.shape[1]
    ones = jnp.where(diagonal(size, size, 0), 1.0, 0.0).astype(x.dtype)
    return lax.dot_general(
        ones, x, (((1,), (1,)), ((), ())), preferred_element_type=jnp.float32
    ).astype(x.dtype)


def make_kernel(n_trade, n_path, side, n_set, trades, per_path, factors):
    offsets = grid_offsets(side)
    n_along = n_path - 1
    count = n_set // 2
    sub = count // 2
    rows = n_trade * sub
    width = DATES * K
    path_steps = sorted(range(1, n_path), key=lambda k: (2, 4, 3, 5, 6, 7, 1).index(k))
    early = n_trade // 2 + 1
    tall = trades // LANES
    f32, bf16 = jnp.float32, jnp.bfloat16

    def kernel(
        coef_hbm, basis_hbm, owner_hbm, slot_hbm, factor_hbm, level_hbm, date_hbm, disc_hbm,
        alloc_ref, cva_ref,
        coef, coef_t, basis, basis_other, basis_t, where, sets, date, disc, dated, dated_other, excess, weights,
        cva_mine, cva_in, al_mine, al_in, part, arrived, gmine, gall,
        in_sem, s1, r1, sd, rd, s3, r3, sc, rc, sa, ra,
    ):
        me = lax.axis_index("trade")
        lane = lax.axis_index("path")
        core = lax.rem(lane, 2)
        partner = lane + 1 - 2 * core
        me_a, me_b = me // side, lax.rem(me, side)
        others = [
            lax.rem(me_a + a, side) * side + lax.rem(me_b + b, side) for a, b in offsets
        ]
        on_path = [lax.rem(lane + k, n_path) for k in path_steps]

        across = [{"trade": o, "path": partner} for o in others]
        first, first_sent = count * core, count * (1 - core)

        loads = [
            pltpu.make_async_copy(src, dst, in_sem.at[i])
            for src, dst, i in (
                (owner_hbm, where.at[0], 0), (slot_hbm, where.at[1], 0), (coef_hbm, coef, 1),
                (basis_hbm, basis, 2), (factor_hbm, sets.at[0], 3), (level_hbm, sets.at[1], 3),
                (disc_hbm, disc, 4), (date_hbm, date, 5),
            )
        ]
        barrier = pltpu.get_barrier_semaphore()
        for there in across:
            pl.semaphore_signal(barrier, inc=1, device_id=there, device_id_type=MESH)
        for k, q in zip(path_steps, on_path):
            if k % 2 == 0:
                pl.semaphore_signal(barrier, inc=1, device_id={"path": q}, device_id_type=MESH)
        for y in range(1, n_path // 2):
            q = lax.rem(partner + 2 * y, n_path)
            pl.semaphore_signal(barrier, inc=1, device_id={"path": q}, device_id_type=MESH)
        for load in loads:
            load.start()

        def send(src, dst, send_sem, recv_sem, device):
            pltpu.make_async_remote_copy(
                src_ref=src, dst_ref=dst, send_sem=send_sem, recv_sem=recv_sem,
                device_id=device, device_id_type=MESH,
            ).start()

        arrive(where, in_sem.at[0])
        loc = where[1] - first_sent
        ids = jnp.where(
            (loc >= 0) & (loc < count), (loc // sub) * rows + where[0] * sub + lax.rem(loc, sub), -1
        )
        which = lax.broadcasted_iota(jnp.int32, (2 * rows, LANES), 0)
        places = lax.broadcasted_iota(jnp.int32, (rows, LANES), 0).astype(f32).astype(bf16)
        one, none = jnp.ones((rows, LANES), bf16), jnp.zeros((rows, LANES), bf16)
        local = [
            jnp.where((ids >= h * rows) & (ids < (h + 1) * rows), ids - h * rows, -1).astype(f32)
            for h in range(2)
        ]

        def picked(h, r):
            row = jnp.broadcast_to(local[h][r : r + 1, :], (16, LANES)).astype(bf16)
            return jnp.where(places == jnp.concatenate([row] * (rows // 16)), one, none)

        arrive(coef, in_sem.at[1])
        deep = tall // 2
        sums = 0.0
        for q in range(2):
            tile = jnp.concatenate(
                [
                    jnp.concatenate([picked(h, r) for r in range(q * deep, (q + 1) * deep)], axis=1)
                    for h in range(2)
                ]
            )
            sums = sums + jnp.dot(
                tile, coef[q * deep * LANES : (q + 1) * deep * LANES, :],
                preferred_element_type=f32,
            )
        part[...] = sums.astype(bf16).reshape(2, n_trade, sub, width)

        arrive(basis, in_sem.at[2])
        pl.semaphore_wait(barrier, n_trade + n_path - 2)
        for h in range(2):
            for j, (o, there) in enumerate(zip(others, across)):
                group = 0
                send(part.at[h, o], arrived.at[h, j], s1.at[0], r1.at[h], there)
        send(basis, basis_other, sd.at[0], rd.at[0], {"path": partner})

        arrive(sets, in_sem.at[3])
        arrive(disc, in_sem.at[4])
        limit = level_step * jnp.sum(
            jnp.where(diagonal(count, n_set, first), sets[1].astype(f32), 0.0),
            axis=1, keepdims=True,
        )
        wanted = jnp.sum(
            jnp.where(diagonal(n_set, n_set, 0), sets[0].astype(f32), 0.0),
            axis=1, keepdims=True,
        )
        pick = lax.broadcasted_iota(jnp.int32, (n_set, factors), 1).astype(f32) == wanted
        pick = jnp.where(pick, 1.0, 0.0).astype(bf16)
        arrive(date, in_sem.at[5])
        dated[...] = jnp.dot(
            pick, date[...].astype(f32).astype(bf16), preferred_element_type=f32
        ).reshape(2, count, per_path)
        send(dated.at[1 - core], dated_other, sd.at[1], rd.at[1], {"path": partner})
        coef_t[...] = turned(coef[...])
        basis_t[0] = turned(basis[...])
        arrive(basis_other, rd.at[0])
        basis_t[1] = turned(basis_other[...])
        arrive(dated_other, rd.at[1])

        moment_of = lax.broadcasted_iota(jnp.int32, (sub, width), 1) // K
        for h in range(2):
            some_sets = slice(h * sub, (h + 1) * sub)
            total = jnp.zeros((sub, width), f32)
            for group, some in ((0, range(n_trade)),):
                arrive(arrived.at[h, some.start : some.stop], r1.at[h])
                for j in some:
                    total = total + arrived[h, j].astype(f32)
            high = total.astype(bf16)
            low = (total - high.astype(f32)).astype(bf16)
            nothing = jnp.zeros_like(high)
            stack = jnp.concatenate(
                [jnp.where(moment_of == d, x, nothing) for x in (high, low) for d in range(DATES)]
            )
            grads = 0.0
            for i, (b_ref, when) in enumerate(
                ((basis, dated[core, some_sets]), (basis_other, dated_other[some_sets]))
            ):
                b = b_ref[...]
                netted = jnp.dot(stack, b, preferred_element_type=f32)
                netted = netted[: DATES * sub] + netted[DATES * sub :]
                slopes = []
                for d in range(DATES):
                    x = netted[d * sub : (d + 1) * sub] - limit[some_sets]
                    e = jnp.exp(-jnp.abs(x))
                    inv = 1.0 / (1.0 + e)
                    sig = jnp.where(x >= 0, inv, e * inv)
                    factor_d = disc[0:1, d : d + 1] / (per_path * n_path)
                    weight = jnp.where(when == float(d), factor_d, 0.0)
                    excess[h, DATES * i + d] = x
                    weights[h, DATES * i + d] = weight
                    slopes.append(weight * sig)
                grads = grads + jnp.dot(
                    jnp.concatenate(slopes).astype(bf16), basis_t[i], preferred_element_type=f32
                )
            grad = jnp.zeros((sub, width), f32)
            for d in range(DATES):
                grad = grad + jnp.where(moment_of == d, grads[d * sub : (d + 1) * sub], 0.0)
            gmine[h] = grad.astype(bf16)
            for o in [0, 10, 6, 9, 11, 14, 2, 5, 7, 8, 13, 15, 1, 3, 4, 12]:
                there = {"trade": o, "path": partner}
                send(gmine.at[h], gall.at[h, me], s3.at[0], r3.at[h], there)
        cvas = []
        for h in range(2):
            cva = jnp.zeros((sub, per_path), f32)
            for i in range(2 * DATES):
                x = excess[h, i]
                plus = jnp.maximum(x, 0.0) + jnp.log1p(jnp.exp(-jnp.abs(x)))
                cva = cva + weights[h, i] * plus
            cvas.append(jnp.sum(cva, axis=1, keepdims=True))
        cva = jnp.concatenate(cvas)
        cva_mine[...] = jnp.sum(
            jnp.where(diagonal(count, n_set, first), cva, 0.0), axis=0, keepdims=True
        )
        for j, q in enumerate(on_path):
            send(cva_mine, cva_in.at[j], sc.at[0], rc.at[0], {"path": q})

        block = 2 * LANES
        for h in range(2):
            arrive(gall.at[h], r3.at[h])
            g = gall[h].reshape(rows, width)
            which = lax.broadcasted_iota(jnp.int32, (rows, LANES), 0) + h * rows
            for r in range(trades // block):
                dots = jnp.dot(
                    g, coef_t[:, r * block : (r + 1) * block], preferred_element_type=f32
                )
                for i in range(2):
                    at = 2 * r + i
                    hit = which == ids[at : at + 1, :]
                    share = jnp.sum(
                        jnp.where(hit, dots[:, i * LANES : (i + 1) * LANES], 0.0),
                        axis=0, keepdims=True,
                    )
                    if h == 0:
                        al_mine[at // 8, at % 8 : at % 8 + 1, :] = share
                    else:
                        al_mine[at // 8, at % 8 : at % 8 + 1, :] += share
                if h == 1 and (2 * r + 2) % 8 == 0:
                    i = (2 * r + 2) // 8 - 1
                    for j, q in enumerate(on_path):
                        send(al_mine.at[i], al_in.at[i, j], sa.at[0], ra.at[i], {"path": q})
        arrive(arrived, s1.at[0])
        arrive(arrived, s3.at[0])
        arrive(basis, sd.at[0])
        arrive(dated_other, sd.at[1])
        arrive(cva_in, sc.at[0])


        arrive(cva_in, rc.at[0])
        cva_total = cva_mine[...]
        for j in range(n_along):
            cva_total = cva_total + cva_in[j]
        cva_ref[...] = cva_total
        for i in range(tall // 8):
            arrive(al_in.at[i], ra.at[i])
            total_alloc = al_mine[i]
            for j in range(n_along):
                total_alloc = total_alloc + al_in[i, j]
            alloc_ref[i * 8 : (i + 1) * 8] = total_alloc
        arrive(al_in, sa.at[0])

    return kernel


def write_out(alloc, cva, alloc_out, cva_out, sem):
    copies = [
        pltpu.make_async_copy(src, dst, sem.at[i])
        for i, (src, dst) in enumerate(((alloc, alloc_out), (cva, cva_out)))
    ]
    for copy in copies:
        copy.start()
    for copy in copies:
        copy.wait()


def solution(mesh):
    n_trade, n_path = mesh.shape["trade"], mesh.shape["path"]
    side = 4

    def on_device(
        coefficients, path_basis, trade_owner, trade_slot, set_factor, set_level, default_date,
        discount,
    ):
        trades, width = coefficients.shape
        n_set = set_factor.shape[0]
        factors, per_path = default_date.shape
        tall = trades // LANES
        half = n_set // 2
        bf16, f32, i32 = jnp.bfloat16, jnp.float32, jnp.int32
        dma = pltpu.SemaphoreType.DMA
        alloc, cva = pl.pallas_call(
            make_kernel(n_trade, n_path, side, n_set, trades, per_path, factors),
            out_shape=(pltpu.VMEM((tall, LANES), f32), pltpu.VMEM((1, n_set), f32)),
            in_specs=[pl.BlockSpec(memory_space=pl.ANY)] * 8,
            out_specs=(
                pl.BlockSpec(memory_space=pltpu.VMEM),
                pl.BlockSpec(memory_space=pltpu.VMEM),
            ),
            scratch_shapes=[
                pltpu.VMEM((trades, width), bf16),
                pltpu.VMEM((width, trades), bf16),
                pltpu.VMEM((width, per_path), bf16),
                pltpu.VMEM((width, per_path), bf16),
                pltpu.VMEM((2, per_path, width), bf16),
                pltpu.VMEM((2, tall, LANES), i32),
                pltpu.VMEM((2, 1, n_set), i32),
                pltpu.VMEM((factors, per_path), i32),
                pltpu.VMEM((1, DATES), f32),
                pltpu.VMEM((2, half, per_path), f32),
                pltpu.VMEM((half, per_path), f32),
                pltpu.VMEM((2, 2 * DATES, half // 2, per_path), f32),
                pltpu.VMEM((2, 2 * DATES, half // 2, per_path), f32),
                pltpu.VMEM((1, n_set), f32),
                pltpu.VMEM((n_path - 1, 1, n_set), f32),
                pltpu.VMEM((tall // 8, 8, LANES), f32),
                pltpu.VMEM((tall // 8, n_path - 1, 8, LANES), f32),
                pltpu.VMEM((2, n_trade, half // 2, width), bf16),
                pltpu.VMEM((2, n_trade, half // 2, width), bf16),
                pltpu.VMEM((2, half // 2, width), bf16),
                pltpu.VMEM((2, n_trade, half // 2, width), bf16),
                dma((6,)),
                dma((1,)),
                dma((2,)),
                dma((2,)),
                dma((2,)),
                dma((1,)),
                dma((2,)),
                dma((1,)),
                dma((1,)),
                dma((1,)),
                dma((2,)),
            ],
            compiler_params=pltpu.CompilerParams(collective_id=0, has_side_effects=True),
        )(
            coefficients,
            path_basis,
            trade_owner.reshape(tall, LANES),
            trade_slot.reshape(tall, LANES),
            set_factor.reshape(1, n_set),
            set_level.reshape(1, n_set),
            default_date,
            discount.reshape(1, DATES),
        )
        alloc, cva = pl.pallas_call(
            write_out,
            out_shape=(
                jax.ShapeDtypeStruct((tall, LANES), f32),
                jax.ShapeDtypeStruct((1, n_set), f32),
            ),
            in_specs=[pl.BlockSpec(memory_space=pltpu.VMEM)] * 2,
            out_specs=(
                pl.BlockSpec(memory_space=pltpu.HBM),
                pl.BlockSpec(memory_space=pltpu.HBM),
            ),
            scratch_shapes=[dma((2,))],
            compiler_params=pltpu.CompilerParams(vmem_limit_bytes=1 << 20),
        )(alloc, cva)
        return alloc.reshape(trades), cva.reshape(n_set)

    return jax.shard_map(
        on_device,
        mesh=mesh,
        in_specs=(
            P("trade", None),
            P(None, "path"),
            P("trade", None),
            P("trade"),
            P("trade"),
            P("trade"),
            P(None, "path"),
            P(),
        ),
        out_specs=(P("trade"), P("trade")),
        check_vma=False,
    )
```
